256 devices in a mesh: expert: 64 (over x_lo, z, y), tensor: 4 (over x_hi, core).
Axes of the slice: x: 4 (x_hi: 2, x_lo: 2; x = x_hi * 2 + x_lo), y: 4, z: 8, core: 2. Of those that a mesh axis runs over, the one named last changes fastest.
Arguments:
- tokens: bfloat16 [8192, 2048], P('expert', 'tensor'), may hold values from -6 to 6
- grad_out: bfloat16 [8192, 2048], P('expert', 'tensor'), may hold values from -6 to 6
- route_weights: float32 [8192, 8], P('expert'), may hold values from 0.02 to 0.5
- expert_ids: int32 [8192, 8], P('expert'), may hold values from 0 to 127, all different within a row; in each aligned block of 128 rows (0 to 127, 128 to 255, ...) at most 12 rows name the same one
- gate_weight: bfloat16 [128, 2048, 768], P('expert', None, 'tensor'), may hold values from -0.125 to 0.125
- up_weight: bfloat16 [128, 2048, 768], P('expert', None, 'tensor'), may hold values from -0.125 to 0.125
- down_weight: bfloat16 [128, 768, 2048], P('expert', 'tensor'), may hold values from -0.21875 to 0.21875
- gate_adapter_first: bfloat16 [128, 2048, 64], P('expert'), may hold values from -0.125 to 0.125
- gate_adapter_second: bfloat16 [128, 64, 768], P('expert', None, 'tensor'), may hold values from -0.75 to 0.75
- up_adapter_first: bfloat16 [128, 2048, 64], P('expert'), may hold values from -0.125 to 0.125
- up_adapter_second: bfloat16 [128, 64, 768], P('expert', None, 'tensor'), may hold values from -0.75 to 0.75
- down_adapter_first: bfloat16 [128, 768, 64], P('expert', 'tensor'), may hold values from -0.21875 to 0.21875
- down_adapter_second: bfloat16 [128, 64, 2048], P('expert'), may hold values from -0.75 to 0.75
Outputs:
- grad_tokens: bfloat16 [8192, 2048], P('expert', 'tensor')
- gate_first_gradient: float32 [128, 2048, 64], P('expert', 'tensor')
- gate_second_gradient: float32 [128, 64, 768], P('expert', None, 'tensor')
- up_first_gradient: float32 [128, 2048, 64], P('expert', 'tensor')
- up_second_gradient: float32 [128, 64, 768], P('expert', None, 'tensor')
- down_first_gradient: float32 [128, 768, 64], P('expert', 'tensor')
- down_second_gradient: float32 [128, 64, 2048], P('expert', None, 'tensor')
The draws below stay inside these ranges and needn't reach their ends.
Inputs may be any that keep to these rules, and one draw needn't show every extreme that they name: `expert_ids`: each token names 8 different experts. Among the 128 rows of one device no expert is named more than 12 times, a bound that some block reaches.
All inputs are finite; a program needn't handle non-finite values.
Results may differ from the reference program's by a relative error of at most 0.012.
Values may be sent and summed in bfloat16 or wider, within the bound.
A program may use at most 128 MiB of HBM per device.

```python
import math
import jax
import jax.numpy as jnp
import numpy as np
from jax import lax

D = 2048
FF = 768
TOP = 8
R = 64
TOK_DEV = 128
EXPERTS = 128
CAP = 12
TOKENS = 8192
N_EXPERT = 64
N_TENSOR = 4


def block_scale(key, extent, pieces, least, high):
    factor_of = 1.0
    for dim, blocks in pieces:
        draws = jax.random.uniform(jax.random.fold_in(jax.random.fold_in(key, 6), dim), (blocks,), jnp.float32, least / len(pieces), high / len(pieces))
        factor_of = factor_of * jnp.repeat(jnp.exp(draws), extent[dim] // blocks).reshape((-1,) + (1,) * (len(extent) - 1 - dim))
    return factor_of


def deal_out(rng, own, number, rows, number_of, top, limit, lean):
    sequence = jax.random.permutation(rng, number_of)
    crowded, common = load_shares(number_of, rows * top, limit, lean, True), load_shares(number_of, rows * top, limit, lean, False)
    places = jnp.arange(number_of)

    def named(lengths, rotation):
        used = int((lengths > 0).sum())
        fixed = max(1, used // 4)
        passed = fixed + (places - fixed + rotation * (used - fixed)) % max(1, number_of - fixed)
        return jnp.zeros((number_of,), jnp.int32).at[sequence[jnp.where(places < fixed, places, passed)]].set(jnp.asarray(lengths, jnp.int32))

    lengths = jnp.where(number % 4 == 0, named(crowded, number // 4), named(common, number - number // 4 - 1))
    mixed = jax.random.permutation(jax.random.fold_in(own, 3), number_of)
    donor, sink = mixed[0:number_of // 2 * 2:2], mixed[1:number_of // 2 * 2:2]
    slack = jnp.minimum(lengths[donor] - 1, limit - lengths[sink]) // 2
    slack = jnp.where((donor == sequence[0]) | (sink == sequence[0]) | (lengths[sink] == 0), 0, jnp.maximum(slack, 0))
    passed = jax.random.randint(jax.random.fold_in(own, 4), (number_of // 2,), 0, 1 << 20) % (slack + 1)
    lengths = lengths.at[donor].add(-passed).at[sink].add(passed)
    items = jnp.searchsorted(jnp.cumsum(lengths), jnp.arange(rows * top), side="right").astype(jnp.int32)
    table = items.reshape(top, rows).T
    table = table[jax.random.permutation(jax.random.fold_in(own, 1), rows)]
    rotation = jax.random.randint(jax.random.fold_in(own, 2), (rows, 1), 0, top)
    return jnp.take_along_axis(table, (jnp.arange(top)[None, :] + rotation) % top, axis=1)


def load_shares(number_of, total, limit, skew, full):
    portions = [(1 << 20) // math.isqrt(standing ** skew) + 1 for standing in range(1, number_of + 1)]
    largest = limit if full else min(limit, max(-(-total // number_of), total * portions[0] // sum(portions)))
    least = 1 if total - largest >= number_of - 1 else 0
    given, spare = [largest] + [least] * (number_of - 1), total - largest - least * (number_of - 1)
    while spare > 0:
        free = [i for i in range(1, number_of) if given[i] < largest] or [i for i in range(1, number_of) if given[i] < limit]
        whole, budget = sum([portions[i] for i in free]), spare
        for i in free:
            more = min(limit - given[i], max(1, budget * portions[i] // whole), spare)
            given[i] = given[i] + more
            spare = spare - more
    return np.array(given)


def bell_draw(rng, dims, deviation, reach, shards=(), kind=jnp.bfloat16):
    drawn = jax.random.normal(rng, dims, jnp.float32) * deviation
    if len(shards) > 0:
        drawn = block_scale(rng, dims, shards, -0.22, 0.18) * drawn
    return jnp.clip(drawn, min=-reach, max=reach).astype(kind)


def setup_inputs(seed: int = 0) -> dict:
    key_list = jax.random.split(jax.random.key(seed), 14)
    tokens = bell_draw(key_list[0], (TOKENS, D), 1.0, 6.0, ((0, 64), (1, 4)))
    grad_out = bell_draw(key_list[1], (TOKENS, D), 1.0, 6.0, ((0, 64), (1, 4)))
    route_weights = jnp.clip(jnp.exp(math.log(0.5) - 3.218876 * jax.random.uniform(key_list[2], (TOKENS, TOP), jnp.float32) ** block_scale(key_list[2], (TOKENS, TOP), ((0, 64),), -0.2, 0.2)), 0.02, 0.5)
    expert_ids_keys = jax.random.split(jax.random.fold_in(key_list[3], 1), TOKENS // TOK_DEV)
    expert_ids_turns = jax.random.permutation(jax.random.fold_in(key_list[3], 3), TOKENS // TOK_DEV)
    expert_ids = jax.vmap(lambda own, number: deal_out(jax.random.fold_in(key_list[3], 2), own, number, TOK_DEV, EXPERTS, TOP, CAP, 2))(expert_ids_keys, expert_ids_turns).reshape((TOKENS, TOP))
    gate_weight = bell_draw(key_list[4], (EXPERTS, D, FF), D ** -0.5, 0.125, ((0, 64), (2, 4)))
    up_weight = bell_draw(key_list[5], (EXPERTS, D, FF), D ** -0.5, 0.125, ((0, 64), (2, 4)))
    down_weight = bell_draw(key_list[6], (EXPERTS, FF, D), FF ** -0.5, 0.21875, ((0, 64), (1, 4)))
    gate_adapter_first = bell_draw(key_list[7], (EXPERTS, D, R), D ** -0.5, 0.125, ((0, 64),))
    gate_adapter_second = bell_draw(key_list[8], (EXPERTS, R, FF), R ** -0.5, 0.75, ((0, 64), (2, 4)))
    up_adapter_first = bell_draw(key_list[9], (EXPERTS, D, R), D ** -0.5, 0.125, ((0, 64),))
    up_adapter_second = bell_draw(key_list[10], (EXPERTS, R, FF), R ** -0.5, 0.75, ((0, 64), (2, 4)))
    down_adapter_first = bell_draw(key_list[11], (EXPERTS, FF, R), FF ** -0.5, 0.21875, ((0, 64), (1, 4)))
    down_adapter_second = bell_draw(key_list[12], (EXPERTS, R, D), R ** -0.5, 0.75, ((0, 64),))
    return dict(tokens=tokens, grad_out=grad_out, route_weights=route_weights, expert_ids=expert_ids, gate_weight=gate_weight, up_weight=up_weight, down_weight=down_weight, gate_adapter_first=gate_adapter_first, gate_adapter_second=gate_adapter_second, up_adapter_first=up_adapter_first, up_adapter_second=up_adapter_second, down_adapter_first=down_adapter_first, down_adapter_second=down_adapter_second)


adapter_scale = 0.5


def expert_pass(routed_input, routed_gradient, gate_weight, up_weight, down_weight, gate_adapter_first, gate_adapter_second, up_adapter_first, up_adapter_second, down_adapter_first, down_adapter_second):
    single_float = jnp.float32
    brain_float_half = jnp.bfloat16
    adapter_gate_term = jnp.dot(routed_input, gate_adapter_first, preferred_element_type=single_float).astype(brain_float_half)
    adapter_up_term = jnp.dot(routed_input, up_adapter_first, preferred_element_type=single_float).astype(brain_float_half)
    gate_activation = jnp.dot(routed_input, gate_weight, preferred_element_type=single_float) + adapter_scale * jnp.dot(adapter_gate_term, gate_adapter_second, preferred_element_type=single_float)
    up_activation = jnp.dot(routed_input, up_weight, preferred_element_type=single_float) + adapter_scale * jnp.dot(adapter_up_term, up_adapter_second, preferred_element_type=single_float)
    sigma = jax.nn.sigmoid(gate_activation)
    active = gate_activation * sigma
    hidden_activation = (active * up_activation).astype(brain_float_half)
    down_adapter_term = jnp.dot(hidden_activation, down_adapter_first, preferred_element_type=single_float).astype(brain_float_half)
    backward_adapter_term = jnp.dot(routed_gradient, down_adapter_second.T, preferred_element_type=single_float).astype(brain_float_half)
    hidden_gradient = jnp.dot(routed_gradient, down_weight.T, preferred_element_type=single_float) + adapter_scale * jnp.dot(backward_adapter_term, down_adapter_first.T, preferred_element_type=single_float)
    gate_gradient = (hidden_gradient * up_activation * sigma * (1.0 + gate_activation * (1.0 - sigma))).astype(brain_float_half)
    up_gradient = (hidden_gradient * active).astype(brain_float_half)
    gate_backward = jnp.dot(gate_gradient, gate_adapter_second.T, preferred_element_type=single_float).astype(brain_float_half)
    up_backward = jnp.dot(up_gradient, up_adapter_second.T, preferred_element_type=single_float).astype(brain_float_half)
    grads = (
        adapter_scale * jnp.dot(routed_input.T, gate_backward, preferred_element_type=single_float),
        adapter_scale * jnp.dot(adapter_gate_term.T, gate_gradient, preferred_element_type=single_float),
        adapter_scale * jnp.dot(routed_input.T, up_backward, preferred_element_type=single_float),
        adapter_scale * jnp.dot(adapter_up_term.T, up_gradient, preferred_element_type=single_float),
        adapter_scale * jnp.dot(hidden_activation.T, backward_adapter_term, preferred_element_type=single_float),
        adapter_scale * jnp.dot(down_adapter_term.T, routed_gradient, preferred_element_type=single_float),
    )
    block_width = FF // N_TENSOR
    total = jnp.zeros((routed_input.shape[0], D), single_float)
    for block in range(N_TENSOR):
        lower = block * block_width
        upper = lower + block_width
        gate_portion = jnp.dot(gate_gradient[:, lower:upper], gate_adapter_second[:, lower:upper].T, preferred_element_type=single_float).astype(brain_float_half)
        up_portion = jnp.dot(up_gradient[:, lower:upper], up_adapter_second[:, lower:upper].T, preferred_element_type=single_float).astype(brain_float_half)
        merged_result = jnp.dot(gate_gradient[:, lower:upper], gate_weight[:, lower:upper].T, preferred_element_type=single_float)
        merged_result = merged_result + jnp.dot(up_gradient[:, lower:upper], up_weight[:, lower:upper].T, preferred_element_type=single_float)
        merged_result = merged_result + adapter_scale * (jnp.dot(gate_portion, gate_adapter_first.T, preferred_element_type=single_float) + jnp.dot(up_portion, up_adapter_first.T, preferred_element_type=single_float))
        total = total + merged_result.astype(brain_float_half).astype(single_float)
    return grads, total


def reference(tokens, grad_out, route_weights, expert_ids, gate_weight, up_weight, down_weight, gate_adapter_first, gate_adapter_second, up_adapter_first, up_adapter_second, down_adapter_first, down_adapter_second):
    single_float = jnp.float32
    brain_float_half = jnp.bfloat16
    blocks = expert_ids.reshape(N_EXPERT, TOK_DEV, TOP)
    numbers = jnp.arange(EXPERTS, dtype=jnp.int32)
    picked = jnp.any(blocks[:, :, :, None] == numbers[None, None, None, :], axis=2).astype(jnp.int32)
    before = jnp.cumsum(picked, axis=1) - picked
    slot_index = jnp.take_along_axis(before, blocks, axis=2).astype(jnp.int32)
    source = jnp.broadcast_to(jnp.arange(N_EXPERT, dtype=jnp.int32)[:, None, None], blocks.shape)
    assigned = jnp.arange(TOKENS * TOP, dtype=jnp.int32).reshape(blocks.shape)
    sentinel = TOKENS * TOP
    table = jnp.full((N_EXPERT, EXPERTS, CAP), sentinel, jnp.int32).at[source, blocks, slot_index].set(assigned)
    per_expert = jnp.transpose(table, (1, 0, 2)).reshape(EXPERTS, N_EXPERT * CAP)
    flat_weights = route_weights.reshape(-1)

    def step(accum, items):
        index, wg, wu, wd, ag, bg, au, bu, ad, bd = items
        live = index < sentinel
        safe = jnp.minimum(index, sentinel - 1)
        token_row = (safe // TOP).astype(jnp.int32)
        routed_input = jnp.where(live[:, None], tokens[token_row].astype(single_float), 0.0).astype(brain_float_half)
        factor = jnp.where(live, flat_weights[safe], 0.0)
        routed_gradient = (factor[:, None] * grad_out[token_row].astype(single_float)).astype(brain_float_half)
        grads, total = expert_pass(routed_input, routed_gradient, wg, wu, wd, ag, bg, au, bu, ad, bd)
        accum = accum.at[token_row].add(jnp.where(live[:, None], total, 0.0))
        return accum, grads

    accum, grads = lax.scan(step, jnp.zeros((TOKENS, D), single_float), (per_expert, gate_weight, up_weight, down_weight, gate_adapter_first, gate_adapter_second, up_adapter_first, up_adapter_second, down_adapter_first, down_adapter_second))
    return (accum.astype(brain_float_half), grads[0], grads[1], grads[2], grads[3], grads[4], grads[5])
```

```python
import functools

import jax
import jax.numpy as jnp
import numpy as np
from jax import lax
from jax.experimental import pallas as pl
from jax.experimental.pallas import tpu as pltpu
from jax.sharding import PartitionSpec as P

MESH = pl.DeviceIdType.MESH
F32 = jnp.float32
BF16 = jnp.bfloat16
PAIRS = ((0, 1), (-1, 2), (-2, 3), (-3, 4))
CAP = 12
FAR = 4096.0
VMEM_LIMIT = 58 * 2**20


def place():
    expert = lax.axis_index("expert")
    tensor = lax.axis_index("tensor")
    y = expert % 4
    z = (expert // 4) % 8
    xl = expert // 32
    xh = tensor // 2
    core = tensor % 2
    return xl, xh, y, z, core


def device(xl, xh, y, z, core):
    return (xl * 32 + z * 4 + y, xh * 2 + core)


def rem_copy(src, dst, send, recv, target):
    return pltpu.make_async_remote_copy(
        src_ref=src, dst_ref=dst, send_sem=send, recv_sem=recv,
        device_id=target, device_id_type=MESH,
    )


def side(xl, xh, step):
    x = (xh * 2 + xl + step) % 4
    return x % 2, x // 2


def greet(targets):
    barrier = pltpu.get_barrier_semaphore()
    for target in targets:
        pl.semaphore_signal(barrier, inc=1, device_id=target, device_id_type=MESH)
    pl.semaphore_wait(barrier, len(targets))


def one_hot(table, base, info_a, info_b, pos_only):
    ids = table + base
    hot = jnp.zeros((48, 256), F32)
    weight = jnp.zeros((48, 256), F32)
    for k in range(8):
        pos = jnp.concatenate([info_a[k : k + 1], info_b[k : k + 1] + FAR], axis=1)
        match = ids == pos
        hot = jnp.where(match, 1.0, hot)
        if not pos_only:
            w = jnp.concatenate([info_a[8 + k : 9 + k], info_b[8 + k : 9 + k]], axis=1)
            weight = jnp.where(match, w, weight)
    if pos_only:
        return hot
    return hot, jnp.sum(weight, axis=1, keepdims=True)


def dispatch_kernel(
    tok_ref, grad_ref, ids_ref, rw_ref, table_ref,
    f_ref, info_ref,
    zb, stage_same, stage_diff, relay,
    info_send, info_recv, swap_sem, ring_send, ring_recv,
    same_send, same_recv, diff_send, diff_recv, x_send, x_recv, core_send, core_recv,
):
    xl, xh, y, z, core = place()
    here = functools.partial(device, xl, xh)
    z_others = [here(y, (z + d) % 8, core) for d in range(1, 8)]
    y_others = [here((y + j) % 4, z, core) for j in range(1, 4)]
    x_sides = [device(*side(xl, xh, s), y, z, core) for s in (1, 3)]
    x_far = device(xl, 1 - xh, y, z, core)
    partner = here(y, z, 1 - core)

    zb[0, 0, :, 0:512] = tok_ref[...]
    zb[0, 0, :, 512:1024] = grad_ref[...]

    ids = ids_ref[...]
    numbers = lax.broadcasted_iota(jnp.int32, (128, 128), 0)
    picked = jnp.zeros((128, 128), F32)
    for k in range(8):
        picked = jnp.where(ids[k : k + 1] == numbers, 1.0, picked)
    later = lax.broadcasted_iota(jnp.int32, (128, 128), 1) > numbers
    before = jnp.dot(
        picked.astype(BF16), jnp.where(later, 1.0, 0.0).astype(BF16), preferred_element_type=F32
    )
    for k in range(8):
        slot = jnp.sum(jnp.where(ids[k : k + 1] == numbers, before, 0.0), axis=0, keepdims=True)
        info_ref[0, k : k + 1, :] = ids[k : k + 1].astype(F32) * CAP + slot
    info_ref[0, 8:16, :] = rw_ref[...]

    greet(z_others + y_others + x_sides + [x_far, partner])

    swap = rem_copy(zb.at[0, 0], zb.at[0, 1], swap_sem.at[0], swap_sem.at[1], x_far)
    swap.start()
    down, up = here(y, (z + 7) % 8, core), here(y, (z + 1) % 8, core)

    def ring(direction, h, chunk):
        if direction == 0:
            src, dst = (h - 1) % 8, h % 8
        else:
            src, dst = (1 - h) % 8, (-h) % 8
        n = (h - 1) * 2 + chunk
        return rem_copy(
            zb.at[src, chunk], zb.at[dst, chunk],
            ring_send.at[direction, n], ring_recv.at[direction, n],
            down if direction == 0 else up,
        )

    ring(0, 1, 0).start()
    ring(1, 1, 0).start()
    infos = []
    for d in range(1, 8):
        copy = rem_copy(
            info_ref.at[0], info_ref.at[(8 - d) % 8], info_send.at[d - 1], info_recv.at[d - 1],
            z_others[d - 1],
        )
        copy.start()
        infos.append(copy)
    swap.wait_recv()
    ring(0, 1, 1).start()
    ring(1, 1, 1).start()
    for copy in infos:
        copy.wait_recv()

    def advance(direction, h, chunk):
        ring(direction, h, chunk).wait_recv()
        nxt = h + 1
        if nxt < 4 or (nxt == 4 and chunk == direction):
            ring(direction, nxt, chunk).start()

    def same_copy(p, j):
        ys = (y + j) % 4
        return rem_copy(
            stage_same.at[p, j - 1], f_ref.at[core, :, :, p, xl, y],
            same_send.at[p, j - 1], same_recv.at[p, j - 1], here(ys, z, core),
        )

    def diff_copy(p, j):
        ys = (y + j) % 4
        return rem_copy(
            stage_diff.at[p, j - 1], relay.at[p, :, y],
            diff_send.at[p, j - 1], diff_recv.at[p, j - 1], here(ys, z, core),
        )

    def x_copy(p, s):
        return rem_copy(
            relay.at[p], f_ref.at[core, xh, :, p, xl],
            x_send.at[p, s], x_recv.at[p, s], x_sides[s],
        )

    def core_copy(p, part):
        if part == 0:
            piece = f_ref.at[core, :, :, p, xl]
        else:
            from_xl, from_xh = side(xl, xh, (1, 3)[part - 1])
            piece = f_ref.at[core, from_xh, :, p, from_xl]
        return rem_copy(piece, piece, core_send.at[p, part], core_recv.at[p, part], partner)

    table = table_ref[...]

    def select(p):
        a, b = PAIRS[p][0] % 8, PAIRS[p][1] % 8
        info_a, info_b = info_ref[a], info_ref[b]
        own = jnp.concatenate([zb[a, 0], zb[b, 0]], axis=0)
        other = jnp.concatenate([zb[a, 1], zb[b, 1]], axis=0)

        def rows_of(hot, weight, x):
            rows = jnp.dot(hot.astype(BF16), x, preferred_element_type=F32)
            taken = rows[:, 0:512].astype(BF16)
            scaled = (rows[:, 512:1024] * weight).astype(BF16)
            return jnp.concatenate([taken, scaled], axis=1)

        for diff in (True, False):
            target_xl = 1 - xl if diff else xl
            hots, weights = [], []
            for j in range(4):
                base = ((target_xl * 64 + z * 8 + ((y + j) % 4) * 2) * CAP).astype(F32)
                hot, weight = one_hot(table, base, info_a, info_b, False)
                hots.append(hot)
                weights.append(weight)
            hot = jnp.concatenate(hots, axis=0)
            weight = jnp.concatenate(weights, axis=0)
            rows = rows_of(hot, weight, own).reshape(4, 2, 24, 1024)
            if diff:
                relay[p, :, y] = rows[0]
                for j in range(1, 4):
                    stage_diff[p, j - 1] = rows[j]
                    diff_copy(p, j).start()
            else:
                rows_b = rows_of(hot, weight, other).reshape(4, 2, 24, 1024)
                f_ref[core, xh, :, p, xl, y] = rows[0]
                f_ref[core, 1 - xh, :, p, xl, y] = rows_b[0]
                for j in range(1, 4):
                    stage_same[p, j - 1, xh] = rows[j]
                    stage_same[p, j - 1, 1 - xh] = rows_b[j]
                    same_copy(p, j).start()

    def forward(p):
        for j in range(1, 4):
            diff_copy(p, j).wait_recv()
        x_copy(p, 0).start()
        x_copy(p, 1).start()
        for j in range(1, 4):
            same_copy(p, j).wait_recv()
        core_copy(p, 0).start()

    def gather(p):
        for s in (0, 1):
            x_copy(p, 1 - s).wait_recv()
            core_copy(p, 1 + s).start()

    advance(0, 1, 0)
    advance(1, 1, 0)
    advance(0, 1, 1)
    advance(1, 1, 1)
    select(0)
    for h in (2, 3):
        advance(0, h, 0)
        advance(1, h, 0)
        advance(0, h, 1)
        advance(1, h, 1)
        select(h - 1)
        forward(h - 2)
        if h == 3:
            gather(0)
    ring(0, 4, 0).wait_recv()
    ring(1, 4, 1).wait_recv()
    select(3)
    forward(2)
    gather(1)
    forward(3)
    gather(2)
    gather(3)
    for p in range(4):
        for part in range(3):
            core_copy(p, part).wait_recv()

    swap.wait_send()
    for copy in infos:
        copy.wait_send()
    for direction in (0, 1):
        for h in range(1, 5):
            for chunk in (0, 1):
                if h < 4 or chunk == direction:
                    ring(direction, h, chunk).wait_send()
    for p in range(4):
        for j in range(1, 4):
            same_copy(p, j).wait_send()
            diff_copy(p, j).wait_send()
        for s in (0, 1):
            x_copy(p, s).wait_send()
        for part in range(3):
            core_copy(p, part).wait_send()


def dispatch(tokens, grad_out, ids, weights, table):
    vmem = pl.BlockSpec(memory_space=pltpu.VMEM)
    dma = pltpu.SemaphoreType.DMA
    return pl.pallas_call(
        dispatch_kernel,
        name="dispatch",
        out_shape=(
            jax.ShapeDtypeStruct((2, 2, 2, 4, 2, 4, 24, 1024), BF16),
            jax.ShapeDtypeStruct((8, 16, 128), F32),
        ),
        in_specs=[vmem] * 5,
        out_specs=(vmem, vmem),
        scratch_shapes=[
            pltpu.VMEM((8, 2, 128, 1024), BF16),
            pltpu.VMEM((4, 3, 2, 2, 24, 1024), BF16),
            pltpu.VMEM((4, 3, 2, 24, 1024), BF16),
            pltpu.VMEM((4, 2, 4, 24, 1024), BF16),
            dma((7,)), dma((7,)), dma((2,)), dma((2, 8)), dma((2, 8)),
            dma((4, 3)), dma((4, 3)), dma((4, 3)), dma((4, 3)),
            dma((4, 2)), dma((4, 2)), dma((4, 3)), dma((4, 3)),
        ],
        compiler_params=pltpu.CompilerParams(
            collective_id=0, has_side_effects=True, vmem_limit_bytes=VMEM_LIMIT
        ),
    )(tokens, grad_out, ids, weights, table)


def nt(a, b):
    return lax.dot_general(a, b, (((1,), (1,)), ((), ())), preferred_element_type=F32)


def tn(a, b):
    return lax.dot_general(a, b, (((0,), (0,)), ((), ())), preferred_element_type=F32)


def nn(a, b):
    return jnp.dot(a, b, preferred_element_type=F32)


PT = 2


def expert_kernel(
    f_ref, wg_ref, wu_ref, wd_ref, ag_ref, bg_ref, au_ref, bu_ref, ad_ref, bd_ref,
    p_ref, low_ref, gs_ref, us_ref, df_ref,
):
    rows = PT * 192

    def tile(n, carry):
        e, h = n // (4 // PT), n % (4 // PT)

        def take(cq, qh, lo):
            return f_ref[cq, qh, e, pl.ds(h * PT, PT), :, :, :, lo : lo + 512].reshape(rows, 512)

        x = jnp.concatenate([take(0, 0, 0), take(1, 0, 0), take(0, 1, 0), take(1, 1, 0)], axis=1)
        lg = nn(x, ag_ref[e]).astype(BF16)
        lu = nn(x, au_ref[e]).astype(BF16)
        gate = nn(x, wg_ref[e]) + 0.5 * nn(lg, bg_ref[e])
        up = nn(x, wu_ref[e]) + 0.5 * nn(lu, bu_ref[e])
        sigma = jax.nn.sigmoid(gate)
        active = gate * sigma
        hidden = (active * up).astype(BF16)
        down = nn(hidden, ad_ref[e]).astype(BF16)
        g = jnp.concatenate(
            [take(0, 0, 512), take(1, 0, 512), take(0, 1, 512), take(1, 1, 512)], axis=1
        )
        back = nt(g, bd_ref[e]).astype(BF16)
        gh = nt(g, wd_ref[e]) + 0.5 * nt(back, ad_ref[e])
        gg = (gh * up * sigma * (1.0 + gate * (1.0 - sigma))).astype(BF16)
        gu = (gh * active).astype(BF16)
        gp = nt(gg, bg_ref[e]).astype(BF16)
        upp = nt(gu, bu_ref[e]).astype(BF16)
        low_ref[e, pl.ds(h * rows, rows), 0:64] = down
        low_ref[e, pl.ds(h * rows, rows), 64:128] = gp
        low_ref[e, pl.ds(h * rows, rows), 128:192] = upp
        gs, us, df = 0.5 * tn(lg, gg), 0.5 * tn(lu, gu), 0.5 * tn(hidden, back)

        @pl.when(h == 0)
        def _():
            gs_ref[e] = gs
            us_ref[e] = us
            df_ref[e] = df

        @pl.when(h > 0)
        def _():
            gs_ref[e] += gs
            us_ref[e] += us
            df_ref[e] += df

        hgp, hup = gp * 0.5, upp * 0.5
        for q in range(4):
            cols = slice(q * 512, q * 512 + 512)
            part = nt(gg, wg_ref[e, cols]) + nt(gu, wu_ref[e, cols])
            part = part + (nt(hgp, ag_ref[e, cols]) + nt(hup, au_ref[e, cols]))
            p_ref[q % 2, q // 2, e, pl.ds(h * PT, PT)] = part.astype(BF16).reshape(PT, 2, 4, 24, 512)
        return carry

    lax.fori_loop(0, 2 * (4 // PT), tile, 0)


def experts(f, wg, wu, wd, ag, bg, au, bu, ad, bd):
    vmem = pl.BlockSpec(memory_space=pltpu.VMEM)
    return pl.pallas_call(
        expert_kernel,
        name="experts",
        out_shape=(
            jax.ShapeDtypeStruct((2, 2, 2, 4, 2, 4, 24, 512), BF16),
            jax.ShapeDtypeStruct((2, 768, 192), BF16),
            jax.ShapeDtypeStruct((2, 64, 192), F32),
            jax.ShapeDtypeStruct((2, 64, 192), F32),
            jax.ShapeDtypeStruct((2, 192, 64), F32),
        ),
        in_specs=[vmem] * 10,
        out_specs=(vmem,) * 5,
        compiler_params=pltpu.CompilerParams(vmem_limit_bytes=VMEM_LIMIT),
    )(f, wg, wu, wd, ag, bg, au, bu, ad, bd)


def return_kernel(
    p_ref, low_ref, f_ref, info_ref, table_ref,
    out_ref, gf_ref, uf_ref, ds_ref,
    r1, cps, cpx, xr, xs_stage, ys, yd, zs, zr, fin, rl, ls, rl2, tl,
    c_send, c_recv, s_send, s_recv, x_send, x_recv, d_send, d_recv, z_send, z_recv, l_send, l_recv, f_sem,
):
    xl, xh, y, z, core = place()
    here = functools.partial(device, xl, xh)
    y_others = [here((y + j) % 4, z, core) for j in range(1, 4)]
    x_sides = [device(*side(xl, xh, s), y, z, core) for s in (1, 3)]
    x_far = device(xl, 1 - xh, y, z, core)
    partner = here(y, z, 1 - core)
    down, up = here(y, (z + 7) % 8, core), here(y, (z + 1) % 8, core)
    greet([down, up] + y_others + x_sides + [x_far, partner])

    def core_copy(p):
        return rem_copy(
            p_ref.at[1 - core, :, :, p], r1.at[:, :, p], c_send.at[p], c_recv.at[p], partner
        )

    low_core = rem_copy(low_ref.at[1 - core], rl, l_send.at[0], l_recv.at[0], partner)
    low_far = rem_copy(ls, rl2, l_send.at[1], l_recv.at[1], x_far)
    low_back = rem_copy(tl.at[core], tl.at[core], l_send.at[2], l_recv.at[2], partner)
    core_copy(3).start()
    core_copy(2).start()
    low_core.start()
    core_copy(1).start()
    core_copy(0).start()

    def same_copy(p, j):
        return rem_copy(
            cps.at[p, j - 1], ys.at[p, y], s_send.at[p, j - 1], s_recv.at[p, j - 1],
            here((y + j) % 4, z, core),
        )

    def diff_copy(p, j):
        return rem_copy(
            xs_stage.at[p, j - 1], yd.at[p, y], d_send.at[p, j - 1], d_recv.at[p, j - 1],
            here((y + j) % 4, z, core),
        )

    def x_copy(p, s):
        _, to_xh = side(xl, xh, (1, 3)[s])
        return rem_copy(
            cpx.at[p, to_xh], xr.at[p, xh], x_send.at[p, s], x_recv.at[p, s], x_sides[s]
        )

    def chip_sum(p):
        core_copy(p).wait_recv()
        for qh in (0, 1):
            mine = p_ref[core, qh, :, p, 1 - xl].astype(F32)
            cpx[p, qh] = (mine + r1[qh, :, p, 1 - xl].astype(F32)).astype(BF16)
        x_copy(p, 0).start()
        x_copy(p, 1).start()
        for j in range(4):
            to = (y + j) % 4
            mine = p_ref[core, :, :, p, xl, to].astype(F32)
            total = (mine + r1[:, :, p, xl, to].astype(F32)).astype(BF16)
            if j == 0:
                ys[p, y] = total
            else:
                cps[p, j - 1] = total
                same_copy(p, j).start()

    def x_sum(p):
        x_copy(p, 0).wait_recv()
        x_copy(p, 1).wait_recv()
        for j in range(4):
            to = (y + j) % 4
            total = (xr[p, 0, :, to].astype(F32) + xr[p, 1, :, to].astype(F32)).astype(BF16)
            if j == 0:
                yd[p, y] = total
            else:
                xs_stage[p, j - 1] = total
                diff_copy(p, j).start()

    table = table_ref[...]

    def combine(p):
        a, b = PAIRS[p][0] % 8, PAIRS[p][1] % 8
        info_a, info_b = info_ref[a], info_ref[b]
        hot = []
        for target_xl in (xl, 1 - xl):
            hots = []
            for j in range(4):
                base = ((target_xl * 64 + z * 8 + j * 2) * CAP).astype(F32)
                hots.append(one_hot(table, base, info_a, info_b, True))
            hot.append(jnp.concatenate(hots, axis=0).astype(BF16))
        for j in range(1, 4):
            same_copy(p, j).wait_recv()
            diff_copy(p, j).wait_recv()
        own = tn(hot[0], ys[p, :, xh].reshape(192, 512)) + tn(hot[1], yd[p].reshape(192, 512))
        other = tn(hot[0], ys[p, :, 1 - xh].reshape(192, 512))
        return {PAIRS[p][0]: (own[0:128], other[0:128]), PAIRS[p][1]: (own[128:], other[128:])}

    def z_copy(direction, h):
        n = direction * 4 + h - 1
        to = up if direction == 0 else down
        if h == 1:
            src, dst = zs.at[n, direction], zr.at[n, direction]
        else:
            src, dst = zs.at[n], zr.at[n]
        return rem_copy(src, dst, z_send.at[n], z_recv.at[n], to)

    def z_hop(direction, h, parts):
        n = direction * 4 + h - 1
        for chunk in (0, 1):
            if h == 1 and chunk != direction:
                continue
            value = parts[chunk]
            if h > 2 or (h == 2 and chunk == direction):
                value = value + zr[n - 1, chunk].astype(F32)
            zs[n, chunk] = value.astype(BF16)
        z_copy(direction, h).start()

    chip_sum(3)
    chip_sum(2)
    low_core.wait_recv()
    ls[...] = (low_ref[core].astype(F32) + rl[...].astype(F32)).astype(BF16)
    low_far.start()
    x_sum(3)
    chip_sum(1)
    chip_sum(0)
    x_sum(2)
    far = combine(3)
    z_hop(0, 1, far[4])
    z_hop(1, 1, far[4])
    x_sum(1)
    low_far.wait_recv()
    tl[core] = (ls[...].astype(F32) + rl2[...].astype(F32)).astype(BF16)
    low_back.start()
    near = combine(2)
    z_copy(0, 1).wait_recv()
    z_hop(0, 2, near[3])
    z_copy(1, 1).wait_recv()
    z_hop(1, 2, far[-3])
    x_sum(0)
    far = near
    near = combine(1)
    z_copy(0, 2).wait_recv()
    z_hop(0, 3, near[2])
    z_copy(1, 2).wait_recv()
    z_hop(1, 3, far[-2])
    far = near
    near = combine(0)
    z_copy(0, 3).wait_recv()
    z_hop(0, 4, near[1])
    z_copy(1, 3).wait_recv()
    z_hop(1, 4, far[-1])

    low_back.wait_recv()
    for e in (0, 1):
        quarter = f_ref[core, xh, e].reshape(768, 1024)
        total = tl[e]
        both = 0.5 * tn(quarter[:, 0:512], total[:, 64:192])
        gf_ref[e] = both[:, 0:64]
        uf_ref[e] = both[:, 64:128]
        ds_ref[e] = 0.5 * tn(total[:, 0:64], quarter[:, 512:1024])

    z_copy(0, 4).wait_recv()
    z_copy(1, 4).wait_recv()
    home = [
        near[0][chunk] + zr[3, chunk].astype(F32) + zr[7, chunk].astype(F32) for chunk in (0, 1)
    ]
    fin[0] = home[1].astype(BF16)
    last = rem_copy(fin.at[0], fin.at[1], f_sem.at[0], f_sem.at[1], x_far)
    last.start()
    last.wait_recv()
    out_ref[...] = (home[0] + fin[1].astype(F32)).astype(BF16)

    last.wait_send()
    low_core.wait_send()
    low_far.wait_send()
    low_back.wait_send()
    for p in range(4):
        core_copy(p).wait_send()
        x_copy(p, 0).wait_send()
        x_copy(p, 1).wait_send()
        for j in range(1, 4):
            same_copy(p, j).wait_send()
            diff_copy(p, j).wait_send()
        z_copy(0, p + 1).wait_send()
        z_copy(1, p + 1).wait_send()


def send_back(p, low, f, info, table):
    vmem = pl.BlockSpec(memory_space=pltpu.VMEM)
    dma = pltpu.SemaphoreType.DMA
    return pl.pallas_call(
        return_kernel,
        name="send_back",
        out_shape=(
            jax.ShapeDtypeStruct((128, 512), BF16),
            jax.ShapeDtypeStruct((2, 512, 64), F32),
            jax.ShapeDtypeStruct((2, 512, 64), F32),
            jax.ShapeDtypeStruct((2, 64, 512), F32),
        ),
        in_specs=[vmem] * 5,
        out_specs=(vmem,) * 4,
        scratch_shapes=[
            pltpu.VMEM((2, 2, 4, 2, 4, 24, 512), BF16),
            pltpu.VMEM((4, 3, 2, 2, 24, 512), BF16),
            pltpu.VMEM((4, 2, 2, 4, 24, 512), BF16),
            pltpu.VMEM((4, 2, 2, 4, 24, 512), BF16),
            pltpu.VMEM((4, 3, 2, 24, 512), BF16),
            pltpu.VMEM((4, 4, 2, 2, 24, 512), BF16),
            pltpu.VMEM((4, 4, 2, 24, 512), BF16),
            pltpu.VMEM((8, 2, 128, 512), BF16),
            pltpu.VMEM((8, 2, 128, 512), BF16),
            pltpu.VMEM((2, 128, 512), BF16),
            pltpu.VMEM((768, 192), BF16),
            pltpu.VMEM((768, 192), BF16),
            pltpu.VMEM((768, 192), BF16),
            pltpu.VMEM((2, 768, 192), BF16),
            dma((4,)), dma((4,)), dma((4, 3)), dma((4, 3)), dma((4, 2)), dma((4, 2)),
            dma((4, 3)), dma((4, 3)), dma((8,)), dma((8,)), dma((3,)), dma((3,)), dma((2,)),
        ],
        compiler_params=pltpu.CompilerParams(
            collective_id=1, has_side_effects=True, vmem_limit_bytes=VMEM_LIMIT
        ),
    )(p, low, f, info, table)


def local(tokens, grad_out, route_weights, expert_ids, wg, wu, wd, ag, bg, au, bu, ad, bd):
    row = np.arange(48)
    table = (row // 24) * CAP + row % CAP + FAR * ((row // CAP) % 2)
    table = jnp.asarray(table.reshape(48, 1), F32)
    f, info = dispatch(tokens, grad_out, expert_ids.T, route_weights.T, table)
    p, low, gs, us, df = experts(f, wg, wu, wd, ag, bg, au, bu, ad, bd)
    out, gf, uf, ds = send_back(p, low, f, info, table)
    return out, gf, gs, uf, us, df, ds


def solution(mesh):
    specs = (
        P("expert", "tensor"), P("expert", "tensor"), P("expert", None), P("expert", None),
        P("expert", None, "tensor"), P("expert", None, "tensor"), P("expert", "tensor", None),
        P("expert", None, None), P("expert", None, "tensor"), P("expert", None, None),
        P("expert", None, "tensor"), P("expert", "tensor", None), P("expert", None, None),
    )
    outs = (
        P("expert", "tensor"), P("expert", "tensor", None), P("expert", None, "tensor"),
        P("expert", "tensor", None), P("expert", None, "tensor"), P("expert", "tensor", None),
        P("expert", None, "tensor"),
    )
    return jax.shard_map(local, mesh=mesh, in_specs=specs, out_specs=outs, check_vma=False)
```

```python
import functools

import jax
import jax.numpy as jnp
import numpy as np
from jax import lax
from jax.experimental import pallas as pl
from jax.experimental.pallas import tpu as pltpu
from jax.sharding import PartitionSpec as P

MESH = pl.DeviceIdType.MESH
F32 = jnp.float32
BF16 = jnp.bfloat16
PAIRS = ((0, 1), (-1, 2), (-3, 4), (-2, 3))
CAP = 12
FAR = 4096.0
VMEM_LIMIT = 67043328


def place():
    expert = lax.axis_index("expert")
    tensor = lax.axis_index("tensor")
    y = expert % 4
    z = (expert // 4) % 8
    xl = expert // 32
    xh = tensor // 2
    core = tensor % 2
    return xl, xh, y, z, core


def device(xl, xh, y, z, core):
    return (xl * 32 + z * 4 + y, xh * 2 + core)


def rem_copy(src, dst, send, recv, target):
    return pltpu.make_async_remote_copy(
        src_ref=src, dst_ref=dst, send_sem=send, recv_sem=recv,
        device_id=target, device_id_type=MESH,
    )


def side(xl, xh, step):
    x = (xh * 2 + xl + step) % 4
    return x % 2, x // 2


def greet(targets):
    barrier = pltpu.get_barrier_semaphore()
    for target in targets:
        pl.semaphore_signal(barrier, inc=1, device_id=target, device_id_type=MESH)
    pl.semaphore_wait(barrier, len(targets))


def nt(a, b):
    return lax.dot_general(a, b, (((1,), (1,)), ((), ())), preferred_element_type=F32)


def tn(a, b):
    return lax.dot_general(a, b, (((0,), (0,)), ((), ())), preferred_element_type=F32)


def nn(a, b):
    return jnp.dot(a, b, preferred_element_type=F32)


def one_hot(ids, positions, weights):
    hot = jnp.zeros((96, 256), F32)
    weight = jnp.zeros((96, 256), F32)
    for k in range(8):
        match = ids == positions[k : k + 1]
        hot = jnp.where(match, 1.0, hot)
        if weights is not None:
            weight = jnp.where(match, weights[k : k + 1], weight)
    if weights is None:
        return hot.astype(BF16)
    return hot.astype(BF16), jnp.sum(weight, axis=1, keepdims=True)


def kernel(
    tok_ref, grad_ref, ids_ref, rw_ref, table_ref,
    wg_hbm, wu_hbm, wd_hbm, ag_hbm, bg_hbm, au_hbm, bu_hbm, ad_hbm, bd_hbm,
    out_ref, gf_ref, gs_ref, uf_ref, us_ref, df_ref, ds_ref,
    wg_ref, wu_ref, wd_ref, ag_ref, bg_ref, au_ref, bu_ref, ad_ref, bd_ref, w_sem,
    info_ref, zb, stage_same, stage_diff, relay, f_ref,
    p_ref, r1, cps, cpx, xr, xs_stage, ys, yd, t_ref, zs, zr, fin, low_ref, rl, ls, rl2, tl,
    info_send, info_recv, swap_sem, ring_send, ring_recv,
    same_send, same_recv, diff_send, diff_recv, x_send, x_recv, core_send, core_recv,
    pc_send, pc_recv, ps_send, ps_recv, px_send, px_recv, pd_send, pd_recv,
    z_send, z_recv, l_send, l_recv, f_sem,
):
    xl, xh, y, z, core = place()
    here = functools.partial(device, xl, xh)
    z_others = [here(y, (z + d) % 8, core) for d in range(1, 8)]
    y_others = [here((y + j) % 4, z, core) for j in range(1, 4)]
    x_sides = [device(*side(xl, xh, s), y, z, core) for s in (1, 3)]
    x_far = device(xl, 1 - xh, y, z, core)
    partner = here(y, z, 1 - core)
    down, up = here(y, (z + 7) % 8, core), here(y, (z + 1) % 8, core)

    loads = []
    for n, (src, dst) in enumerate((
        (wg_hbm, wg_ref), (wu_hbm, wu_ref), (wd_hbm, wd_ref), (ag_hbm, ag_ref), (bg_hbm, bg_ref),
        (au_hbm, au_ref), (bu_hbm, bu_ref), (ad_hbm, ad_ref), (bd_hbm, bd_ref),
    )):
        load = pltpu.make_async_copy(src, dst, w_sem.at[n])
        load.start()
        loads.append(load)

    zb[0, 0, :, 0:512] = tok_ref[...]
    zb[0, 0, :, 512:1024] = grad_ref[...]

    ids = ids_ref[...]
    numbers = lax.broadcasted_iota(jnp.int32, (128, 128), 0)
    picked = jnp.zeros((128, 128), F32)
    for k in range(8):
        picked = jnp.where(ids[k : k + 1] == numbers, 1.0, picked)
    later = lax.broadcasted_iota(jnp.int32, (128, 128), 1) > numbers
    before = nn(picked.astype(BF16), jnp.where(later, 1.0, 0.0).astype(BF16))
    for k in range(8):
        slot = jnp.sum(jnp.where(ids[k : k + 1] == numbers, before, 0.0), axis=0, keepdims=True)
        info_ref[0, k : k + 1, :] = ids[k : k + 1].astype(F32) * CAP + slot
    info_ref[0, 8:16, :] = rw_ref[...]

    greet(z_others + y_others + x_sides + [x_far, partner])

    swap = rem_copy(zb.at[0, 0], zb.at[0, 1], swap_sem.at[0], swap_sem.at[1], x_far)
    swap.start()

    def ring(direction, h, chunk):
        if direction == 0:
            src, dst = (h - 1) % 8, h % 8
        else:
            src, dst = (1 - h) % 8, (-h) % 8
        n = (h - 1) * 2 + chunk
        return rem_copy(
            zb.at[src, chunk], zb.at[dst, chunk],
            ring_send.at[direction, n], ring_recv.at[direction, n],
            down if direction == 0 else up,
        )

    ring(0, 1, 0).start()
    ring(1, 1, 0).start()
    infos = []
    for d in range(1, 8):
        copy = rem_copy(
            info_ref.at[0], info_ref.at[(8 - d) % 8], info_send.at[d - 1], info_recv.at[d - 1],
            z_others[d - 1],
        )
        copy.start()
        infos.append(copy)
    swap.wait_recv()
    ring(0, 1, 1).start()
    ring(1, 1, 1).start()
    for copy in infos:
        copy.wait_recv()

    def advance(h):
        for chunk in (0, 1):
            for direction in (0, 1):
                if h == 4 and chunk != direction:
                    continue
                ring(direction, h, chunk).wait_recv()
                if h < 3 or (h == 3 and chunk == direction):
                    ring(direction, h + 1, chunk).start()

    def same_copy(p, e, j):
        return rem_copy(
            stage_same.at[p, e, j - 1], f_ref.at[core, :, e, p, xl, y],
            same_send.at[p, e, j - 1], same_recv.at[p, e, j - 1], here((y + j) % 4, z, core),
        )

    def diff_copy(p, e, j):
        return rem_copy(
            stage_diff.at[p, e, j - 1], relay.at[p, e, y],
            diff_send.at[p, e, j - 1], diff_recv.at[p, e, j - 1], here((y + j) % 4, z, core),
        )

    def x_copy(p, e, s):
        return rem_copy(
            relay.at[p, e], f_ref.at[core, xh, e, p, xl],
            x_send.at[p, e, s], x_recv.at[p, e, s], x_sides[s],
        )

    def core_copy(p, e, part):
        if part == 0:
            piece = f_ref.at[core, :, e, p, xl]
        else:
            from_xl, from_xh = side(xl, xh, (1, 3)[part - 1])
            piece = f_ref.at[core, from_xh, e, p, from_xl]
        return rem_copy(piece, piece, core_send.at[p, e, part], core_recv.at[p, e, part], partner)

    def pc_copy(p, e):
        return rem_copy(
            p_ref.at[1 - core, :, e, p], r1.at[:, e, p], pc_send.at[p, e], pc_recv.at[p, e], partner
        )

    def ps_copy(p, e, j):
        return rem_copy(
            cps.at[p, e, j - 1], ys.at[p, :, e, y], ps_send.at[p, e, j - 1], ps_recv.at[p, e, j - 1],
            here((y + j) % 4, z, core),
        )

    def pd_copy(p, e, j):
        return rem_copy(
            xs_stage.at[p, e, j - 1], yd.at[p, e, y], pd_send.at[p, e, j - 1], pd_recv.at[p, e, j - 1],
            here((y + j) % 4, z, core),
        )

    def px_copy(p, e, s):
        _, to_xh = side(xl, xh, (1, 3)[s])
        return rem_copy(
            cpx.at[p, e, to_xh], xr.at[p, e, xh], px_send.at[p, e, s], px_recv.at[p, e, s], x_sides[s]
        )

    def z_copy(direction, h, chunk):
        n = direction * 4 + h - 1
        return rem_copy(
            zs.at[n, chunk], zr.at[n, chunk], z_send.at[n, chunk], z_recv.at[n, chunk],
            up if direction == 0 else down,
        )

    low_core = rem_copy(low_ref.at[1 - core], rl, l_send.at[0], l_recv.at[0], partner)
    low_far = rem_copy(ls, rl2, l_send.at[1], l_recv.at[1], x_far)
    low_back = rem_copy(tl.at[core], tl.at[core], l_send.at[2], l_recv.at[2], partner)

    table = table_ref[...]

    def row_ids(target_xl, e, first):
        return jnp.concatenate(
            [
                table + ((target_xl * 64 + z * 8 + ((first + j) % 4) * 2 + e) * CAP).astype(F32)
                for j in range(4)
            ],
            axis=0,
        )

    def pair_info(p, weights):
        a, b = PAIRS[p][0] % 8, PAIRS[p][1] % 8
        positions = jnp.concatenate([info_ref[a, 0:8], info_ref[b, 0:8] + FAR], axis=1)
        if not weights:
            return positions, None
        return positions, jnp.concatenate([info_ref[a, 8:16], info_ref[b, 8:16]], axis=1)

    def select(p):
        a, b = PAIRS[p][0] % 8, PAIRS[p][1] % 8
        positions, weights = pair_info(p, True)
        own = jnp.concatenate([zb[a, 0], zb[b, 0]], axis=0)
        other = jnp.concatenate([zb[a, 1], zb[b, 1]], axis=0)

        def rows_of(hot, weight, x):
            rows = nn(hot, x)
            taken = rows[:, 0:512].astype(BF16)
            scaled = (rows[:, 512:1024] * weight).astype(BF16)
            return jnp.concatenate([taken, scaled], axis=1).reshape(4, 24, 1024)

        for e in (0, 1):
            hot, weight = one_hot(row_ids(1 - xl, e, y), positions, weights)
            rows = rows_of(hot, weight, own)
            relay[p, e, y] = rows[0]
            for j in range(1, 4):
                stage_diff[p, e, j - 1] = rows[j]
                diff_copy(p, e, j).start()
            hot, weight = one_hot(row_ids(xl, e, y), positions, weights)
            rows = rows_of(hot, weight, own)
            rows_b = rows_of(hot, weight, other)
            f_ref[core, xh, e, p, xl, y] = rows[0]
            f_ref[core, 1 - xh, e, p, xl, y] = rows_b[0]
            for j in range(1, 4):
                stage_same[p, e, j - 1, xh] = rows[j]
                stage_same[p, e, j - 1, 1 - xh] = rows_b[j]
                same_copy(p, e, j).start()

    def forward(u):
        p, e = u // 2, u % 2
        for j in range(1, 4):
            diff_copy(p, e, j).wait_recv()
        x_copy(p, e, 0).start()
        x_copy(p, e, 1).start()
        for j in range(1, 4):
            same_copy(p, e, j).wait_recv()
        core_copy(p, e, 0).start()

    def gather(u):
        p, e = u // 2, u % 2
        for s in (0, 1):
            x_copy(p, e, 1 - s).wait_recv()
            core_copy(p, e, 1 + s).start()

    def compute(u):
        p, e = u // 2, u % 2
        for part in range(3):
            core_copy(p, e, part).wait_recv()

        def take(cq, qh, lo):
            return f_ref[cq, qh, e, p, :, :, :, lo : lo + 512].reshape(192, 512)

        x = jnp.concatenate([take(0, 0, 0), take(1, 0, 0), take(0, 1, 0), take(1, 1, 0)], axis=1)
        gate_in = jnp.concatenate([wg_ref[e], ag_ref[e]], axis=0)
        up_in = jnp.concatenate([wu_ref[e], au_ref[e]], axis=0)
        down_in = jnp.concatenate([wd_ref[e], bd_ref[e]], axis=0)
        gate = nt(x, gate_in)
        lg = gate[:, 192:256].astype(BF16)
        gate = gate[:, 0:192] + 0.5 * nn(lg, bg_ref[e])
        up_part = nt(x, up_in)
        lu = up_part[:, 192:256].astype(BF16)
        up_part = up_part[:, 0:192] + 0.5 * nn(lu, bu_ref[e])
        sigma = jax.nn.sigmoid(gate)
        active = gate * sigma
        hidden = (active * up_part).astype(BF16)
        down_part = nt(hidden, ad_ref[e]).astype(BF16)
        g = jnp.concatenate(
            [take(0, 0, 512), take(1, 0, 512), take(0, 1, 512), take(1, 1, 512)], axis=1
        )
        gh = nt(g, down_in)
        back = gh[:, 192:256].astype(BF16)
        gh = gh[:, 0:192] + 0.5 * nn(back, ad_ref[e])
        gg = (gh * up_part * sigma * (1.0 + gate * (1.0 - sigma))).astype(BF16)
        gu = (gh * active).astype(BF16)
        gp = nt(gg, bg_ref[e]).astype(BF16)
        upp = nt(gu, bu_ref[e]).astype(BF16)
        left = jnp.concatenate([gg, gp * 0.5], axis=1)
        right = jnp.concatenate([gu, upp * 0.5], axis=1)
        for q in range(4):
            cols = slice(q * 512, q * 512 + 512)
            part = nn(left, gate_in[:, cols]) + nn(right, up_in[:, cols])
            p_ref[q % 2, q // 2, e, p] = part.astype(BF16).reshape(2, 4, 24, 512)
        pc_copy(p, e).start()
        rows = slice(p * 192, p * 192 + 192)
        low_ref[e, rows, 0:64] = down_part
        low_ref[e, rows, 64:128] = gp
        low_ref[e, rows, 128:192] = upp
        for ref, value in ((gs_ref, tn(lg, gg)), (us_ref, tn(lu, gu)), (df_ref, tn(back, hidden))):
            if p == 0:
                ref[e] = 0.5 * value
            else:
                ref[e] += 0.5 * value

    def chip_sum(u):
        p, e = u // 2, u % 2
        pc_copy(p, e).wait_recv()
        for qh in (0, 1):
            mine = p_ref[core, qh, e, p, 1 - xl].astype(F32)
            cpx[p, e, qh] = (mine + r1[qh, e, p, 1 - xl].astype(F32)).astype(BF16)
        px_copy(p, e, 0).start()
        px_copy(p, e, 1).start()
        for j in range(4):
            to = (y + j) % 4
            mine = p_ref[core, :, e, p, xl, to].astype(F32)
            total = (mine + r1[:, e, p, xl, to].astype(F32)).astype(BF16)
            if j == 0:
                ys[p, :, e, y] = total
            else:
                cps[p, e, j - 1] = total
                ps_copy(p, e, j).start()

    def x_sum(u):
        p, e = u // 2, u % 2
        px_copy(p, e, 0).wait_recv()
        px_copy(p, e, 1).wait_recv()
        for j in range(4):
            to = (y + j) % 4
            total = (xr[p, e, 0, to].astype(F32) + xr[p, e, 1, to].astype(F32)).astype(BF16)
            if j == 0:
                yd[p, e, y] = total
            else:
                xs_stage[p, e, j - 1] = total
                pd_copy(p, e, j).start()

    def combine(p):
        positions, _ = pair_info(p, False)
        hot_same = jnp.concatenate(
            [one_hot(row_ids(xl, e, 0), positions, None) for e in (0, 1)], axis=0
        )
        hot_diff = jnp.concatenate(
            [one_hot(row_ids(1 - xl, e, 0), positions, None) for e in (0, 1)], axis=0
        )
        for e in (0, 1):
            for j in range(1, 4):
                ps_copy(p, e, j).wait_recv()
                pd_copy(p, e, j).wait_recv()
        t_ref[p, 1] = tn(hot_same, ys[p, 1 - xh].reshape(192, 512))
        t_ref[p, 0] = tn(hot_same, ys[p, xh].reshape(192, 512)) + tn(hot_diff, yd[p].reshape(192, 512))

    held = {d: (p, i) for p in range(4) for i, d in enumerate(PAIRS[p])}

    def part_of(distance, chunk):
        p, i = held[distance]
        return t_ref[p, chunk, i * 128 : i * 128 + 128]

    def z_hop(direction, h, chunk):
        if h == 1 and chunk != direction:
            return
        n = direction * 4 + h - 1
        distance = 5 - h
        value = part_of(distance if direction == 0 or h == 1 else -distance, chunk)
        if h > 2 or (h == 2 and chunk == direction):
            z_copy(direction, h - 1, chunk).wait_recv()
            value = value + zr[n - 1, chunk].astype(F32)
        zs[n, chunk] = value.astype(BF16)
        z_copy(direction, h, chunk).start()

    advance(1)
    select(0)
    forward(0)
    advance(2)
    select(1)
    gather(0)
    forward(1)
    for load in loads:
        load.wait()
    compute(0)
    advance(3)
    gather(1)
    forward(2)
    chip_sum(0)
    compute(1)
    x_sum(0)
    advance(4)
    select(2)
    select(3)
    gather(2)
    forward(3)
    for u in range(1, 7):
        chip_sum(u)
        compute(u + 1)
        x_sum(u)
        if u == 4:
            combine(0)
        if u == 6:
            combine(1)
        if u + 2 < 8:
            gather(u + 2)
        if u + 3 < 8:
            forward(u + 3)
    low_core.start()
    chip_sum(7)
    low_core.wait_recv()
    ls[...] = (low_ref[core].astype(F32) + rl[...].astype(F32)).astype(BF16)
    low_far.start()
    combine(2)
    z_hop(0, 1, 0)
    z_hop(1, 1, 1)
    x_sum(7)
    combine(3)
    for chunk in (1, 0):
        z_hop(0, 2, chunk)
        z_hop(1, 2, chunk)
    low_far.wait_recv()
    tl[core] = (ls[...].astype(F32) + rl2[...].astype(F32)).astype(BF16)
    low_back.start()
    for chunk in (1, 0):
        z_hop(0, 3, chunk)
        z_hop(1, 3, chunk)

    low_back.wait_recv()

    def adapters(e):
        quarter = f_ref[core, xh, e].reshape(768, 1024)
        total = tl[e]
        both = 0.5 * tn(total[:, 64:192], quarter[:, 0:512])
        gf_ref[e] = both[0:64]
        uf_ref[e] = both[64:128]
        ds_ref[e] = 0.5 * tn(total[:, 0:64], quarter[:, 512:1024])

    adapters(0)
    for chunk in (1, 0):
        z_hop(0, 4, chunk)
        z_hop(1, 4, chunk)
    adapters(1)

    def home(chunk):
        z_copy(0, 4, chunk).wait_recv()
        z_copy(1, 4, chunk).wait_recv()
        return part_of(0, chunk) + zr[3, chunk].astype(F32) + zr[7, chunk].astype(F32)

    fin[0] = home(1).astype(BF16)
    last = rem_copy(fin.at[0], fin.at[1], f_sem.at[0], f_sem.at[1], x_far)
    last.start()
    mine = home(0)
    last.wait_recv()
    out_ref[...] = (mine + fin[1].astype(F32)).astype(BF16)

    last.wait_send()
    swap.wait_send()
    for copy in infos:
        copy.wait_send()
    low_core.wait_send()
    low_far.wait_send()
    low_back.wait_send()
    for direction in (0, 1):
        for h in range(1, 5):
            for chunk in (0, 1):
                if h < 4 or chunk == direction:
                    ring(direction, h, chunk).wait_send()
                if h > 1 or chunk == direction:
                    z_copy(direction, h, chunk).wait_send()
    for p in range(4):
        for e in (0, 1):
            pc_copy(p, e).wait_send()
            for s in (0, 1):
                x_copy(p, e, s).wait_send()
                px_copy(p, e, s).wait_send()
            for n in range(3):
                same_copy(p, e, n + 1).wait_send()
                diff_copy(p, e, n + 1).wait_send()
                ps_copy(p, e, n + 1).wait_send()
                pd_copy(p, e, n + 1).wait_send()
                core_copy(p, e, n).wait_send()


def step(tokens, grad_out, ids, weights, table, *frozen):
    vmem = pl.BlockSpec(memory_space=pltpu.VMEM)
    hbm = pl.BlockSpec(memory_space=pl.ANY)
    dma = pltpu.SemaphoreType.DMA

    def buf(*shape):
        return pltpu.VMEM(shape, BF16)

    return pl.pallas_call(
        kernel,
        name="experts",
        out_shape=(
            jax.ShapeDtypeStruct((128, 512), BF16),
            jax.ShapeDtypeStruct((2, 64, 512), F32),
            jax.ShapeDtypeStruct((2, 64, 192), F32),
            jax.ShapeDtypeStruct((2, 64, 512), F32),
            jax.ShapeDtypeStruct((2, 64, 192), F32),
            jax.ShapeDtypeStruct((2, 64, 192), F32),
            jax.ShapeDtypeStruct((2, 64, 512), F32),
        ),
        in_specs=[vmem] * 5 + [hbm] * 9,
        out_specs=(vmem,) * 7,
        scratch_shapes=[buf(*w.shape) for w in frozen] + [
            dma((9,)),
            pltpu.VMEM((8, 16, 128), F32),
            buf(8, 2, 128, 1024),
            buf(4, 2, 3, 2, 24, 1024),
            buf(4, 2, 3, 24, 1024),
            buf(4, 2, 4, 24, 1024),
            buf(2, 2, 2, 4, 2, 4, 24, 1024),
            buf(2, 2, 2, 4, 2, 4, 24, 512),
            buf(2, 2, 4, 2, 4, 24, 512),
            buf(4, 2, 3, 2, 24, 512),
            buf(4, 2, 2, 4, 24, 512),
            buf(4, 2, 2, 4, 24, 512),
            buf(4, 2, 3, 24, 512),
            buf(4, 2, 2, 4, 24, 512),
            buf(4, 2, 4, 24, 512),
            pltpu.VMEM((4, 2, 256, 512), F32),
            buf(8, 2, 128, 512),
            buf(8, 2, 128, 512),
            buf(2, 128, 512),
            buf(2, 768, 192),
            buf(768, 192),
            buf(768, 192),
            buf(768, 192),
            buf(2, 768, 192),
            dma((7,)), dma((7,)), dma((2,)), dma((2, 8)), dma((2, 8)),
            dma((4, 2, 3)), dma((4, 2, 3)), dma((4, 2, 3)), dma((4, 2, 3)),
            dma((4, 2, 2)), dma((4, 2, 2)), dma((4, 2, 3)), dma((4, 2, 3)),
            dma((4, 2)), dma((4, 2)), dma((4, 2, 3)), dma((4, 2, 3)),
            dma((4, 2, 2)), dma((4, 2, 2)), dma((4, 2, 3)), dma((4, 2, 3)),
            dma((8, 2)), dma((8, 2)), dma((3,)), dma((3,)), dma((2,)),
        ],
        compiler_params=pltpu.CompilerParams(
            collective_id=0, has_side_effects=True, vmem_limit_bytes=VMEM_LIMIT
        ),
    )(tokens, grad_out, ids, weights, table, *frozen)


def finish_kernel(*refs):
    for src, dst in zip(refs[:7], refs[7:]):
        dst[...] = src[...]


def finish(outs):
    vmem = pl.BlockSpec(memory_space=pltpu.VMEM)
    return pl.pallas_call(
        finish_kernel,
        name="finish",
        out_shape=tuple(jax.ShapeDtypeStruct(o.shape, o.dtype) for o in outs),
        in_specs=[vmem] * 7,
        out_specs=(vmem,) * 7,
    )(*outs)


def local(tokens, grad_out, route_weights, expert_ids, wg, wu, wd, ag, bg, au, bu, ad, bd):
    row = np.arange(24)
    table = row % CAP + FAR * (row // CAP)
    table = jnp.asarray(table.reshape(24, 1), F32)
    wg, wu, ag, au, ad = [jnp.swapaxes(w, 1, 2) for w in (wg, wu, ag, au, ad)]
    outs = step(
        tokens, grad_out, expert_ids.T, route_weights.T, table, wg, wu, wd, ag, bg, au, bu, ad, bd
    )
    out, gf, gs, uf, us, df, ds = finish(outs)
    gf, uf, df = [jnp.swapaxes(w, 1, 2) for w in (gf, uf, df)]
    return out, gf, gs, uf, us, df, ds


def solution(mesh):
    specs = (
        P("expert", "tensor"), P("expert", "tensor"), P("expert", None), P("expert", None),
        P("expert", None, "tensor"), P("expert", None, "tensor"), P("expert", "tensor", None),
        P("expert", None, None), P("expert", None, "tensor"), P("expert", None, None),
        P("expert", None, "tensor"), P("expert", "tensor", None), P("expert", None, None),
    )
    outs = (
        P("expert", "tensor"), P("expert", "tensor", None), P("expert", None, "tensor"),
        P("expert", "tensor", None), P("expert", None, "tensor"), P("expert", "tensor", None),
        P("expert", None, "tensor"),
    )
    return jax.shard_map(local, mesh=mesh, in_specs=specs, out_specs=outs, check_vma=False)
```

```python
import functools

import jax
import jax.numpy as jnp
import numpy as np
from jax import lax
from jax.experimental import pallas as pl
from jax.experimental.pallas import tpu as pltpu
from jax.sharding import PartitionSpec as P

MESH = pl.DeviceIdType.MESH
F32 = jnp.float32
BF16 = jnp.bfloat16
PAIRS = ((0, 1), (-1, 2), (-2, 3), (-3, 4))
CAP = 12
FAR = 4096.0
VMEM_LIMIT = 67043328


def place():
    expert = lax.axis_index("expert")
    tensor = lax.axis_index("tensor")
    y = expert % 4
    z = (expert // 4) % 8
    xl = expert // 32
    xh = tensor // 2
    core = tensor % 2
    return xl, xh, y, z, core


def device(xl, xh, y, z, core):
    return (xl * 32 + z * 4 + y, xh * 2 + core)


def rem_copy(src, dst, send, recv, target):
    return pltpu.make_async_remote_copy(
        src_ref=src, dst_ref=dst, send_sem=send, recv_sem=recv,
        device_id=target, device_id_type=MESH,
    )


def drain(ref, sem):
    pltpu.make_async_copy(ref, ref, sem).wait()


def side(xl, xh, step):
    x = (xh * 2 + xl + step) % 4
    return x % 2, x // 2


def greet(targets):
    barrier = pltpu.get_barrier_semaphore()
    for target in targets:
        pl.semaphore_signal(barrier, inc=1, device_id=target, device_id_type=MESH)
    pl.semaphore_wait(barrier, len(targets))


def nt(a, b):
    return lax.dot_general(a, b, (((1,), (1,)), ((), ())), preferred_element_type=F32)


def tn(a, b):
    return lax.dot_general(a, b, (((0,), (0,)), ((), ())), preferred_element_type=F32)


def nn(a, b):
    return jnp.dot(a, b, preferred_element_type=F32)


def one_hot(ids, positions, weights):
    hot = jnp.zeros((96, 256), F32)
    weight = jnp.zeros((96, 256), F32)
    for k in range(8):
        match = ids == positions[k : k + 1]
        hot = jnp.where(match, 1.0, hot)
        if weights is not None:
            weight = jnp.where(match, weights[k : k + 1], weight)
    if weights is None:
        return hot.astype(BF16)
    return hot.astype(BF16), jnp.sum(weight, axis=1, keepdims=True)


def kernel(
    tok_ref, grad_ref, ids_ref, rw_ref, table_ref,
    wg_hbm, wu_hbm, wd_hbm, ag_hbm, bg_hbm, au_hbm, bu_hbm, ad_hbm, bd_hbm,
    out_ref, gf_ref, gs_ref, uf_ref, us_ref, df_ref, ds_ref,
    wg_ref, wu_ref, wd_ref, ag_ref, bg_ref, au_ref, bu_ref, ad_ref, bd_ref, w_sem,
    info_ref, zb, stage_same, stage_diff, relay, f_ref,
    p_ref, r1, cpx, xr, back_stage, yr, t_ref, zs, zr, low_ref, rl, ls, rl2, tl,
    info_send, info_recv, swap_sem, ring_send, ring_recv,
    same_send, same_recv, diff_send, diff_recv, x_send, x_recv, core_send, core_recv,
    pc_send, pc_recv, px_send, px_recv, pd_send, pd_recv,
    z_send, z_recv, l_send, l_recv, o_sem,
    out_v, gf_v, gs_v, uf_v, us_v, df_v, ds_v,
):
    xl, xh, y, z, core = place()
    here = functools.partial(device, xl, xh)
    y_others = [here((y + j) % 4, z, core) for j in range(1, 4)]
    x_sides = [device(*side(xl, xh, s), y, z, core) for s in (1, 3)]
    x_far = device(xl, 1 - xh, y, z, core)
    partner = here(y, z, 1 - core)
    down, up = here(y, (z + 7) % 8, core), here(y, (z + 1) % 8, core)

    puts = []

    def put(n, src, dst):
        copy = pltpu.make_async_copy(src, dst, o_sem.at[n])
        copy.start()
        puts.append(copy)

    loads = []
    for n, (src, dst) in enumerate((
        (wg_hbm, wg_ref), (wu_hbm, wu_ref), (wd_hbm, wd_ref), (ag_hbm, ag_ref), (bg_hbm, bg_ref),
        (au_hbm, au_ref), (bu_hbm, bu_ref), (ad_hbm, ad_ref), (bd_hbm, bd_ref),
    )):
        load = pltpu.make_async_copy(src, dst, w_sem.at[n])
        load.start()
        loads.append(load)

    zb[0, 0, :, 0:512] = tok_ref[...]
    zb[0, 0, :, 512:1024] = grad_ref[...]

    ids = ids_ref[...]
    numbers = lax.broadcasted_iota(jnp.int32, (128, 128), 0)
    picked = jnp.zeros((128, 128), F32)
    for k in range(8):
        picked = jnp.where(ids[k : k + 1] == numbers, 1.0, picked)
    later = lax.broadcasted_iota(jnp.int32, (128, 128), 1) > numbers
    before = nn(picked.astype(BF16), jnp.where(later, 1.0, 0.0).astype(BF16))
    for k in range(8):
        slot = jnp.sum(jnp.where(ids[k : k + 1] == numbers, before, 0.0), axis=0, keepdims=True)
        info_ref[0, k : k + 1, :] = ids[k : k + 1].astype(F32) * CAP + slot
    info_ref[0, 8:16, :] = rw_ref[...]

    greet([down, up] + y_others + x_sides + [x_far, partner])

    swap = rem_copy(zb.at[0, 0], zb.at[0, 1], swap_sem.at[0], swap_sem.at[1], x_far)
    swap.start()

    def ring(direction, h, chunk):
        if direction == 0:
            src, dst = (h - 1) % 8, h % 8
        else:
            src, dst = (1 - h) % 8, (-h) % 8
        n = (h - 1) * 2 + chunk
        return rem_copy(
            zb.at[src, chunk], zb.at[dst, chunk],
            ring_send.at[0], ring_recv.at[direction, n],
            down if direction == 0 else up,
        )

    def ring_info(direction, h):
        if direction == 0:
            src, dst = (h - 1) % 8, h % 8
        else:
            src, dst = (1 - h) % 8, (-h) % 8
        return rem_copy(
            info_ref.at[src], info_ref.at[dst],
            info_send.at[0], info_recv.at[direction, h - 1],
            down if direction == 0 else up,
        )

    def advance(h, chunk):
        for direction in (0, 1):
            if chunk == 0 and (h < 4 or direction == 0):
                ring_info(direction, h).wait_recv()
                if h < 3 or (h == 3 and direction == 0):
                    ring_info(direction, h + 1).start()
            if h < 4 or chunk == direction:
                ring(direction, h, chunk).wait_recv()
                if h < 3 or (h == 3 and chunk == direction):
                    ring(direction, h + 1, chunk).start()

    for direction in (0, 1):
        ring_info(direction, 1).start()
        ring(direction, 1, 0).start()
    swap.wait_recv()
    ring(0, 1, 1).start()
    ring(1, 1, 1).start()

    def same_copy(p, e, j, chunk):
        qh = xh if chunk == 0 else 1 - xh
        return rem_copy(
            stage_same.at[p, e, j - 1, chunk], f_ref.at[core, qh, e, p, xl, y],
            same_send.at[0], same_recv.at[p, e],
            here((y + j) % 4, z, core),
        )

    def diff_copy(p, e, j):
        return rem_copy(
            stage_diff.at[p, e, j - 1], relay.at[p, e, y],
            diff_send.at[0], diff_recv.at[p, e], here((y + j) % 4, z, core),
        )

    def x_copy(p, e, s):
        return rem_copy(
            relay.at[p, e], f_ref.at[core, xh, e, p, xl],
            x_send.at[s], x_recv.at[p, e, s], x_sides[s],
        )

    def core_copy(p, e, part):
        if part == 0:
            piece = f_ref.at[core, :, e, p, xl]
        else:
            from_xl, from_xh = side(xl, xh, (1, 3)[part - 1])
            piece = f_ref.at[core, from_xh, e, p, from_xl]
        return rem_copy(piece, piece, core_send.at[part], core_recv.at[p, e, part], partner)

    def pc_copy(p, e):
        return rem_copy(
            p_ref.at[1 - core, :, e, p], r1.at[:, e, p], pc_send.at[0], pc_recv.at[p, e], partner
        )

    def pd_copy(p, e, j):
        return rem_copy(
            back_stage.at[p, e, j - 1], yr.at[p, :, e, y], pd_send.at[0], pd_recv.at[p],
            here((y + j) % 4, z, core),
        )

    def px_copy(p, e, s):
        if s == 2:
            src, dst, to = cpx.at[p, e, 2], xr.at[p, e, 2], x_far
        else:
            _, to_xh = side(xl, xh, (1, 3)[s])
            src, dst, to = cpx.at[p, e, to_xh], xr.at[p, e, xh], x_sides[s]
        return rem_copy(src, dst, px_send.at[0], px_recv.at[p, e], to)

    def z_copy(direction, h, chunk):
        n = direction * 4 + h - 1
        return rem_copy(
            zs.at[n, chunk], zr.at[n, chunk], z_send.at[0], z_recv.at[n, chunk],
            up if direction == 0 else down,
        )

    LOW = (slice(0, 576), slice(576, 768))

    def low_core(n):
        return rem_copy(
            low_ref.at[1 - core, LOW[n]], rl.at[LOW[n]], l_send.at[0, n], l_recv.at[0, n], partner
        )

    def low_far(n):
        return rem_copy(ls.at[LOW[n]], rl2.at[LOW[n]], l_send.at[1, n], l_recv.at[1, n], x_far)

    def low_back(n):
        return rem_copy(
            tl.at[core, LOW[n]], tl.at[core, LOW[n]], l_send.at[2, n], l_recv.at[2, n], partner
        )

    def low_chip(n):
        low_core(n).wait_recv()
        rows = LOW[n]
        ls[rows] = (low_ref[core, rows].astype(F32) + rl[rows].astype(F32)).astype(BF16)
        low_far(n).start()

    def low_total(n):
        low_far(n).wait_recv()
        rows = LOW[n]
        tl[core, rows] = (ls[rows].astype(F32) + rl2[rows].astype(F32)).astype(BF16)
        low_back(n).start()

    table = table_ref[...]

    def row_ids(target_xl, e, first):
        return jnp.concatenate(
            [
                table + ((target_xl * 64 + z * 8 + ((first + j) % 4) * 2 + e) * CAP).astype(F32)
                for j in range(4)
            ],
            axis=0,
        )

    def pair_info(p, weights):
        a, b = PAIRS[p][0] % 8, PAIRS[p][1] % 8
        positions = jnp.concatenate([info_ref[a, 0:8], info_ref[b, 0:8] + FAR], axis=1)
        if not weights:
            return positions, None
        return positions, jnp.concatenate([info_ref[a, 8:16], info_ref[b, 8:16]], axis=1)

    def rows_of(hot, weight, p, chunk):
        a, b = PAIRS[p][0] % 8, PAIRS[p][1] % 8
        rows = nn(hot, jnp.concatenate([zb[a, chunk], zb[b, chunk]], axis=0))
        taken = rows[:, 0:512].astype(BF16)
        scaled = (rows[:, 512:1024] * weight).astype(BF16)
        return jnp.concatenate([taken, scaled], axis=1).reshape(4, 24, 1024)

    def select_diff(p, e):
        hot, weight = one_hot(row_ids(1 - xl, e, y), *pair_info(p, True))
        rows = rows_of(hot, weight, p, 0)
        relay[p, e, y] = rows[0]
        for j in range(1, 4):
            stage_diff[p, e, j - 1] = rows[j]
            diff_copy(p, e, j).start()

    def select_same(p, e, chunks):
        hot, weight = one_hot(row_ids(xl, e, y), *pair_info(p, True))
        for chunk in chunks:
            rows = rows_of(hot, weight, p, chunk)
            f_ref[core, xh if chunk == 0 else 1 - xh, e, p, xl, y] = rows[0]
            for j in range(1, 4):
                stage_same[p, e, j - 1, chunk] = rows[j]
                same_copy(p, e, j, chunk).start()

    def select_a(p):
        for e in (0, 1):
            select_diff(p, e)
        for e in (0, 1):
            select_same(p, e, (0,))

    def select_b(p):
        for e in (0, 1):
            select_same(p, e, (1,))

    def select(p):
        for e in (0, 1):
            select_diff(p, e)
        for e in (0, 1):
            select_same(p, e, (0, 1))

    def forward_x(u):
        p, e = u // 2, u % 2
        drain(stage_diff.at[p, e], diff_recv.at[p, e])
        x_copy(p, e, 0).start()
        x_copy(p, e, 1).start()

    def forward_c(u):
        p, e = u // 2, u % 2
        drain(stage_same.at[p, e], same_recv.at[p, e])
        core_copy(p, e, 0).start()

    def forward(u):
        forward_x(u)
        forward_c(u)

    def gather(u):
        p, e = u // 2, u % 2
        for s in (0, 1):
            x_copy(p, e, 1 - s).wait_recv()
            core_copy(p, e, 1 + s).start()

    def compute(u):
        p, e = u // 2, u % 2
        for part in range(3):
            core_copy(p, e, part).wait_recv()

        def take(cq, qh, lo):
            return f_ref[cq, qh, e, p, :, :, :, lo : lo + 512].reshape(192, 512)

        x = jnp.concatenate([take(0, 0, 0), take(1, 0, 0), take(0, 1, 0), take(1, 1, 0)], axis=1)
        gate_in = jnp.concatenate([wg_ref[e], ag_ref[e]], axis=0)
        up_in = jnp.concatenate([wu_ref[e], au_ref[e]], axis=0)
        down_in = jnp.concatenate([wd_ref[e], bd_ref[e]], axis=0)
        gate = nt(x, gate_in)
        lg = gate[:, 192:256].astype(BF16)
        gate = gate[:, 0:192] + 0.5 * nn(lg, bg_ref[e])
        up_part = nt(x, up_in)
        lu = up_part[:, 192:256].astype(BF16)
        up_part = up_part[:, 0:192] + 0.5 * nn(lu, bu_ref[e])
        sigma = jax.nn.sigmoid(gate)
        active = gate * sigma
        hidden = (active * up_part).astype(BF16)
        down_part = nt(hidden, ad_ref[e]).astype(BF16)
        g = jnp.concatenate(
            [take(0, 0, 512), take(1, 0, 512), take(0, 1, 512), take(1, 1, 512)], axis=1
        )
        gh = nt(g, down_in)
        back = gh[:, 192:256].astype(BF16)
        gh = gh[:, 0:192] + 0.5 * nn(back, ad_ref[e])
        gg = (gh * up_part * sigma * (1.0 + gate * (1.0 - sigma))).astype(BF16)
        gu = (gh * active).astype(BF16)
        gp = nt(gg, bg_ref[e]).astype(BF16)
        upp = nt(gu, bu_ref[e]).astype(BF16)
        left = jnp.concatenate([gg, gp * 0.5], axis=1)
        right = jnp.concatenate([gu, upp * 0.5], axis=1)
        for q in range(4):
            cols = slice(q * 512, q * 512 + 512)
            part = nn(left, gate_in[:, cols]) + nn(right, up_in[:, cols])
            p_ref[q % 2, q // 2, e, p] = part.astype(BF16).reshape(2, 4, 24, 512)
        pc_copy(p, e).start()
        rows = slice(p * 192, p * 192 + 192)
        low_ref[e, rows, 0:64] = down_part
        low_ref[e, rows, 64:128] = gp
        low_ref[e, rows, 128:192] = upp
        for ref, value in ((gs_v, tn(lg, gg)), (us_v, tn(lu, gu)), (df_v, tn(back, hidden))):
            if p == 0:
                ref[e] = 0.5 * value
            else:
                ref[e] += 0.5 * value

    def chip_sum(u):
        p, e = u // 2, u % 2
        pc_copy(p, e).wait_recv()
        for n, qh, xs in ((0, 0, 1 - xl), (1, 1, 1 - xl), (2, 1 - xh, xl)):
            mine = p_ref[core, qh, e, p, xs].astype(F32)
            cpx[p, e, n] = (mine + r1[qh, e, p, xs].astype(F32)).astype(BF16)
        for n in range(3):
            px_copy(p, e, n).start()

    def x_sum(u):
        p, e = u // 2, u % 2
        drain(xr.at[p, e], px_recv.at[p, e])
        for j in range(4):
            to = (y + j) % 4
            same = p_ref[core, xh, e, p, xl, to].astype(F32) + r1[xh, e, p, xl, to].astype(F32)
            same = (same + xr[p, e, 2, to].astype(F32)).astype(BF16)
            diff = (xr[p, e, 0, to].astype(F32) + xr[p, e, 1, to].astype(F32)).astype(BF16)
            if j == 0:
                yr[p, 0, e, y] = same
                yr[p, 1, e, y] = diff
            else:
                back_stage[p, e, j - 1, 0] = same
                back_stage[p, e, j - 1, 1] = diff
                pd_copy(p, e, j).start()

    def combine(p):
        positions, _ = pair_info(p, False)
        hot = jnp.concatenate(
            [
                one_hot(row_ids(target_xl, e, 0), positions, None)
                for target_xl in (xl, 1 - xl)
                for e in (0, 1)
            ],
            axis=0,
        )
        drain(back_stage.at[p], pd_recv.at[p])
        t_ref[p] = tn(hot, yr[p].reshape(384, 512))

    held = {d: (p, i) for p in range(4) for i, d in enumerate(PAIRS[p])}

    def part_of(distance, chunk):
        p, i = held[distance]
        return t_ref[p, i * 128 + chunk * 64 : i * 128 + chunk * 64 + 64]

    def z_hop(direction, h, chunk):
        if h == 1 and chunk != direction:
            return
        n = direction * 4 + h - 1
        distance = 5 - h
        value = part_of(distance if direction == 0 or h == 1 else -distance, chunk)
        if h > 2 or (h == 2 and chunk == direction):
            z_copy(direction, h - 1, chunk).wait_recv()
            value = value + zr[n - 1, chunk].astype(F32)
        zs[n, chunk] = value.astype(BF16)
        z_copy(direction, h, chunk).start()


    def adapters(e):
        quarter = f_ref[core, xh, e].reshape(768, 1024)
        total = tl[e]
        both = 0.5 * tn(total[:, 64:192], quarter[:, 0:512])
        gf_v[e] = both[0:64]
        uf_v[e] = both[64:128]
        ds_v[e] = 0.5 * tn(total[:, 0:64], quarter[:, 512:1024])

    advance(1, 0)
    select_a(0)
    forward_x(0)
    forward_x(1)
    advance(1, 1)
    select_b(0)
    gather(0)
    advance(2, 0)
    select_a(1)
    gather(1)
    forward_c(0)
    forward_c(1)
    for load in loads:
        load.wait()
    compute(0)
    forward_x(2)
    advance(2, 1)
    select_b(1)
    forward_x(3)
    compute(1)
    chip_sum(0)
    advance(3, 0)
    gather(2)
    chip_sum(1)
    forward_c(2)
    advance(3, 1)
    select(2)
    gather(3)
    forward_c(3)
    compute(2)
    forward_x(4)
    x_sum(0)
    advance(4, 0)
    advance(4, 1)
    select(3)
    forward_x(5)
    compute(3)
    gather(4)
    forward_c(4)
    x_sum(1)
    chip_sum(2)
    compute(4)
    gather(5)
    forward_c(5)
    forward_x(6)
    chip_sum(3)
    forward_x(7)
    compute(5)
    x_sum(2)
    gather(6)
    forward_c(6)
    chip_sum(4)
    compute(6)
    gather(7)
    forward_c(7)
    x_sum(3)
    chip_sum(5)
    compute(7)
    low_core(0).start()
    low_core(1).start()
    chip_sum(6)
    x_sum(4)
    chip_sum(7)
    for n, (src, dst) in enumerate(((gs_v, gs_ref), (us_v, us_ref), (df_v, df_ref))):
        put(n, src, dst)
    x_sum(5)
    combine(0)
    combine(1)
    x_sum(6)
    x_sum(7)
    low_chip(0)
    low_chip(1)
    combine(2)
    combine(3)
    z_hop(0, 1, 0)
    z_hop(1, 1, 1)
    for chunk in (1, 0):
        z_hop(0, 2, chunk)
        z_hop(1, 2, chunk)
    drain(zb.at[pl.ds(0, 7)], ring_send.at[0])
    drain(info_ref.at[pl.ds(0, 7)], info_send.at[0])
    swap.wait_send()
    drain(stage_same, same_send.at[0])
    drain(stage_diff, diff_send.at[0])
    drain(relay, x_send.at[0])
    drain(relay, x_send.at[1])
    drain(f_ref.at[0, :, :, :, 0], core_send.at[0])
    drain(f_ref.at[0, 0, :, :, 0], core_send.at[1])
    drain(f_ref.at[0, 0, :, :, 0], core_send.at[2])
    for chunk in (1, 0):
        z_hop(0, 3, chunk)
        z_hop(1, 3, chunk)
    low_total(0)
    low_total(1)
    for chunk in (1, 0):
        z_hop(0, 4, chunk)
        z_hop(1, 4, chunk)
    low_back(0).wait_recv()
    low_back(1).wait_recv()
    adapters(0)
    adapters(1)
    for n, (src, dst) in enumerate(((gf_v, gf_ref), (uf_v, uf_ref), (ds_v, ds_ref))):
        put(n + 3, src, dst)

    def home(chunk):
        z_copy(0, 4, chunk).wait_recv()
        z_copy(1, 4, chunk).wait_recv()
        return part_of(0, chunk) + zr[3, chunk].astype(F32) + zr[7, chunk].astype(F32)

    out_v[64:128] = home(1).astype(BF16)
    out_v[0:64] = home(0).astype(BF16)
    put(6, out_v, out_ref)
    drain(zs.at[pl.ds(0, 7)], z_send.at[0])
    drain(back_stage, pd_send.at[0])
    drain(cpx, px_send.at[0])
    drain(p_ref.at[0], pc_send.at[0])
    for n in (0, 1):
        low_core(n).wait_send()
        low_far(n).wait_send()
        low_back(n).wait_send()
    for copy in puts:
        copy.wait()


def step(tokens, grad_out, ids, weights, table, *frozen):
    vmem = pl.BlockSpec(memory_space=pltpu.VMEM)
    hbm = pl.BlockSpec(memory_space=pl.ANY)
    dma = pltpu.SemaphoreType.DMA

    def buf(*shape):
        return pltpu.VMEM(shape, BF16)

    return pl.pallas_call(
        kernel,
        name="experts",
        out_shape=(
            jax.ShapeDtypeStruct((128, 512), BF16),
            jax.ShapeDtypeStruct((2, 64, 512), F32),
            jax.ShapeDtypeStruct((2, 64, 192), F32),
            jax.ShapeDtypeStruct((2, 64, 512), F32),
            jax.ShapeDtypeStruct((2, 64, 192), F32),
            jax.ShapeDtypeStruct((2, 64, 192), F32),
            jax.ShapeDtypeStruct((2, 64, 512), F32),
        ),
        in_specs=[vmem] * 5 + [hbm] * 9,
        out_specs=(hbm,) * 7,
        scratch_shapes=[buf(*w.shape) for w in frozen] + [
            dma((9,)),
            pltpu.VMEM((8, 16, 128), F32),
            buf(8, 2, 128, 1024),
            buf(4, 2, 3, 2, 24, 1024),
            buf(4, 2, 3, 24, 1024),
            buf(4, 2, 4, 24, 1024),
            buf(2, 2, 2, 4, 2, 4, 24, 1024),
            buf(2, 2, 2, 4, 2, 4, 24, 512),
            buf(2, 2, 4, 2, 4, 24, 512),
            buf(4, 2, 3, 4, 24, 512),
            buf(4, 2, 3, 4, 24, 512),
            buf(4, 2, 3, 2, 24, 512),
            buf(4, 2, 2, 4, 24, 512),
            pltpu.VMEM((4, 256, 512), F32),
            buf(8, 2, 64, 512),
            buf(8, 2, 64, 512),
            buf(2, 768, 192),
            buf(768, 192),
            buf(768, 192),
            buf(768, 192),
            buf(2, 768, 192),
            dma((1,)), dma((2, 4)), dma((2,)), dma((1,)), dma((2, 8)),
            dma((1,)), dma((4, 2)), dma((1,)), dma((4, 2)),
            dma((2,)), dma((4, 2, 2)), dma((3,)), dma((4, 2, 3)),
            dma((1,)), dma((4, 2)), dma((1,)), dma((4, 2)), dma((1,)), dma((4,)),
            dma((1,)), dma((8, 2)), dma((3, 2)), dma((3, 2)), dma((7,)),
            buf(128, 512),
            *[pltpu.VMEM(shape, F32) for shape in (
                (2, 64, 512), (2, 64, 192), (2, 64, 512), (2, 64, 192), (2, 64, 192), (2, 64, 512),
            )],
        ],
        compiler_params=pltpu.CompilerParams(
            collective_id=0, has_side_effects=True, vmem_limit_bytes=VMEM_LIMIT
        ),
    )(tokens, grad_out, ids, weights, table, *frozen)


def finish_kernel(*refs):
    for src, dst in zip(refs[:7], refs[7:]):
        dst[...] = src[...]


def finish(outs):
    vmem = pl.BlockSpec(memory_space=pltpu.VMEM)
    return pl.pallas_call(
        finish_kernel,
        name="finish",
        out_shape=tuple(jax.ShapeDtypeStruct(o.shape, o.dtype) for o in outs),
        in_specs=[vmem] * 7,
        out_specs=(vmem,) * 7,
    )(*outs)


def local(tokens, grad_out, route_weights, expert_ids, wg, wu, wd, ag, bg, au, bu, ad, bd):
    row = np.arange(24)
    table = row % CAP + FAR * (row // CAP)
    table = jnp.asarray(table.reshape(24, 1), F32)
    wg, wu, ag, au, ad = [jnp.swapaxes(w, 1, 2) for w in (wg, wu, ag, au, ad)]
    outs = step(
        tokens, grad_out, expert_ids.T, route_weights.T, table, wg, wu, wd, ag, bg, au, bu, ad, bd
    )
    out, gf, gs, uf, us, df, ds = finish(outs)
    gf, uf, df = [jnp.swapaxes(w, 1, 2) for w in (gf, uf, df)]
    return out, gf, gs, uf, us, df, ds


def solution(mesh):
    specs = (
        P("expert", "tensor"), P("expert", "tensor"), P("expert", None), P("expert", None),
        P("expert", None, "tensor"), P("expert", None, "tensor"), P("expert", "tensor", None),
        P("expert", None, None), P("expert", None, "tensor"), P("expert", None, None),
        P("expert", None, "tensor"), P("expert", "tensor", None), P("expert", None, None),
    )
    outs = (
        P("expert", "tensor"), P("expert", "tensor", None), P("expert", None, "tensor"),
        P("expert", "tensor", None), P("expert", None, "tensor"), P("expert", "tensor", None),
        P("expert", None, "tensor"),
    )
    return jax.shard_map(local, mesh=mesh, in_specs=specs, out_specs=outs, check_vma=False)
```

```python
import functools

import jax
import jax.numpy as jnp
import numpy as np
from jax import lax
from jax.experimental import pallas as pl
from jax.experimental.pallas import tpu as pltpu
from jax.sharding import PartitionSpec as P

MESH = pl.DeviceIdType.MESH
F32 = jnp.float32
BF16 = jnp.bfloat16
PAIRS = ((0, 1), (-1, 2), (-2, 3), (-3, 4))
CAP = 12
FAR = 4096.0
VMEM_LIMIT = 67043328


def place():
    expert = lax.axis_index("expert")
    tensor = lax.axis_index("tensor")
    y = expert % 4
    z = (expert // 4) % 8
    xl = expert // 32
    xh = tensor // 2
    core = tensor % 2
    return xl, xh, y, z, core


def device(xl, xh, y, z, core):
    return (xl * 32 + z * 4 + y, xh * 2 + core)


def rem_copy(src, dst, send, recv, target):
    return pltpu.make_async_remote_copy(
        src_ref=src, dst_ref=dst, send_sem=send, recv_sem=recv,
        device_id=target, device_id_type=MESH,
    )


def drain(ref, sem):
    pltpu.make_async_copy(ref, ref, sem).wait()


def side(xl, xh, step):
    x = (xh * 2 + xl + step) % 4
    return x % 2, x // 2


def greet(targets):
    barrier = pltpu.get_barrier_semaphore()
    for target in targets:
        pl.semaphore_signal(barrier, inc=1, device_id=target, device_id_type=MESH)
    pl.semaphore_wait(barrier, len(targets))


def nt(a, b):
    return lax.dot_general(a, b, (((1,), (1,)), ((), ())), preferred_element_type=F32)


def tn(a, b):
    return lax.dot_general(a, b, (((0,), (0,)), ((), ())), preferred_element_type=F32)


def nn(a, b):
    return jnp.dot(a, b, preferred_element_type=F32)


def one_hot(ids, positions, weights):
    hot = jnp.zeros((96, 256), F32)
    weight = jnp.zeros((96, 256), F32)
    for k in range(8):
        match = ids == positions[k : k + 1]
        hot = jnp.where(match, 1.0, hot)
        if weights is not None:
            weight = jnp.where(match, weights[k : k + 1], weight)
    if weights is None:
        return hot.astype(BF16)
    return hot.astype(BF16), jnp.sum(weight, axis=1, keepdims=True)


def kernel(
    tok_ref, grad_ref, ids_ref, rw_ref, table_ref,
    wg_hbm, wu_hbm, wd_hbm, ag_hbm, bg_hbm, au_hbm, bu_hbm, ad_hbm, bd_hbm,
    out_ref, gf_ref, gs_ref, uf_ref, us_ref, df_ref, ds_ref,
    wg_ref, wu_ref, wd_ref, ag_ref, bg_ref, au_ref, bu_ref, ad_ref, bd_ref, w_sem,
    info_ref, zb, stage_same, stage_diff, relay, f_ref,
    p_ref, r1, cpx, xr, back_stage, yr, t_ref, zs, zr, low_ref, rl, ls, rl2, tl,
    info_send, info_recv, swap_sem, ring_send, ring_recv,
    same_send, same_recv, diff_send, diff_recv, x_send, x_recv, core_send, core_recv,
    pc_send, pc_recv, px_send, px_recv, pd_send, pd_recv,
    z_send, z_recv, l_send, l_recv, o_sem,
    out_v, gf_v, gs_v, uf_v, us_v, df_v, ds_v,
):
    xl, xh, y, z, core = place()
    here = functools.partial(device, xl, xh)
    y_others = [here((y + j) % 4, z, core) for j in range(1, 4)]
    x_sides = [device(*side(xl, xh, s), y, z, core) for s in (1, 3)]
    x_far = device(xl, 1 - xh, y, z, core)
    partner = here(y, z, 1 - core)
    down, up = here(y, (z + 7) % 8, core), here(y, (z + 1) % 8, core)

    puts = []

    def put(n, src, dst):
        copy = pltpu.make_async_copy(src, dst, o_sem.at[n])
        copy.start()
        puts.append(copy)

    loads = []
    for n, (src, dst) in enumerate((
        (wg_hbm, wg_ref), (wu_hbm, wu_ref), (wd_hbm, wd_ref), (ag_hbm, ag_ref), (bg_hbm, bg_ref),
        (au_hbm, au_ref), (bu_hbm, bu_ref), (ad_hbm, ad_ref), (bd_hbm, bd_ref),
    )):
        load = pltpu.make_async_copy(src, dst, w_sem.at[n])
        load.start()
        loads.append(load)

    zb[0, 0, :, 0:512] = tok_ref[...]
    zb[0, 0, :, 512:1024] = grad_ref[...]

    ids = ids_ref[...]
    numbers = lax.broadcasted_iota(jnp.int32, (128, 128), 0)
    picked = jnp.zeros((128, 128), F32)
    for k in range(8):
        picked = jnp.where(ids[k : k + 1] == numbers, 1.0, picked)
    later = lax.broadcasted_iota(jnp.int32, (128, 128), 1) > numbers
    before = nn(picked.astype(BF16), jnp.where(later, 1.0, 0.0).astype(BF16))
    for k in range(8):
        slot = jnp.sum(jnp.where(ids[k : k + 1] == numbers, before, 0.0), axis=0, keepdims=True)
        info_ref[0, k : k + 1, :] = ids[k : k + 1].astype(F32) * CAP + slot
    info_ref[0, 8:16, :] = rw_ref[...]

    greet([down, up] + y_others + x_sides + [x_far, partner])

    swap = rem_copy(zb.at[0, 0], zb.at[0, 1], swap_sem.at[0], swap_sem.at[1], x_far)
    swap.start()

    def ring(direction, h, chunk):
        if direction == 0:
            src, dst = (h - 1) % 8, h % 8
        else:
            src, dst = (1 - h) % 8, (-h) % 8
        n = (h - 1) * 2 + chunk
        return rem_copy(
            zb.at[src, chunk], zb.at[dst, chunk],
            ring_send.at[0], ring_recv.at[direction, n],
            down if direction == 0 else up,
        )

    def ring_info(direction, h):
        if direction == 0:
            src, dst = (h - 1) % 8, h % 8
        else:
            src, dst = (1 - h) % 8, (-h) % 8
        return rem_copy(
            info_ref.at[src], info_ref.at[dst],
            info_send.at[0], info_recv.at[direction, h - 1],
            down if direction == 0 else up,
        )

    def advance(h, chunk):
        for direction in (0, 1):
            if chunk == 0 and (h < 4 or direction == 0):
                ring_info(direction, h).wait_recv()
                if h < 3 or (h == 3 and direction == 0):
                    ring_info(direction, h + 1).start()
            if h < 4 or chunk == direction:
                ring(direction, h, chunk).wait_recv()
                if h < 3 or (h == 3 and chunk == direction):
                    ring(direction, h + 1, chunk).start()

    for direction in (0, 1):
        ring_info(direction, 1).start()
        ring(direction, 1, 0).start()
    def same_copy(p, e, j, chunk):
        qh = xh if chunk == 0 else 1 - xh
        return rem_copy(
            stage_same.at[p, e, j - 1, chunk], f_ref.at[core, qh, e, p, xl, y],
            same_send.at[0], same_recv.at[p, e],
            here((y + j) % 4, z, core),
        )

    def diff_copy(p, e, j):
        return rem_copy(
            stage_diff.at[p, e, j - 1], relay.at[p, e, y],
            diff_send.at[0], diff_recv.at[p, e], here((y + j) % 4, z, core),
        )

    def x_copy(p, e, s):
        return rem_copy(
            relay.at[p, e], f_ref.at[core, xh, e, p, xl],
            x_send.at[s], x_recv.at[p, e, s], x_sides[s],
        )

    def core_copy(p, e, part):
        if part == 0:
            piece = f_ref.at[core, :, e, p, xl]
        else:
            from_xl, from_xh = side(xl, xh, (1, 3)[part - 1])
            piece = f_ref.at[core, from_xh, e, p, from_xl]
        return rem_copy(piece, piece, core_send.at[part], core_recv.at[p, e, part], partner)

    def pc_copy(p, e):
        return rem_copy(
            p_ref.at[1 - core, :, e, p], r1.at[:, e, p], pc_send.at[0], pc_recv.at[p, e], partner
        )

    def pd_copy(p, e, j):
        return rem_copy(
            back_stage.at[p, e, j - 1], yr.at[p, :, e, y], pd_send.at[0], pd_recv.at[p],
            here((y + j) % 4, z, core),
        )

    def px_copy(p, e, s):
        if s == 2:
            src, dst, to = cpx.at[p, e, 2], xr.at[p, e, 2], x_far
        else:
            _, to_xh = side(xl, xh, (1, 3)[s])
            src, dst, to = cpx.at[p, e, to_xh], xr.at[p, e, xh], x_sides[s]
        return rem_copy(src, dst, px_send.at[0], px_recv.at[p, e], to)

    def z_copy(direction, h, chunk):
        n = direction * 4 + h - 1
        return rem_copy(
            zs.at[n, chunk], zr.at[n, chunk], z_send.at[0], z_recv.at[n, chunk],
            up if direction == 0 else down,
        )

    LOW = (slice(0, 576), slice(576, 768))

    def low_core(n):
        return rem_copy(
            low_ref.at[1 - core, LOW[n]], rl.at[LOW[n]], l_send.at[0, n], l_recv.at[0, n], partner
        )

    def low_far(n):
        return rem_copy(ls.at[LOW[n]], rl2.at[LOW[n]], l_send.at[1, n], l_recv.at[1, n], x_far)

    def low_back(n):
        return rem_copy(
            tl.at[core, LOW[n]], tl.at[core, LOW[n]], l_send.at[2, n], l_recv.at[2, n], partner
        )

    def low_chip(n):
        low_core(n).wait_recv()
        rows = LOW[n]
        ls[rows] = (low_ref[core, rows].astype(F32) + rl[rows].astype(F32)).astype(BF16)
        low_far(n).start()

    def low_total(n):
        low_far(n).wait_recv()
        rows = LOW[n]
        tl[core, rows] = (ls[rows].astype(F32) + rl2[rows].astype(F32)).astype(BF16)
        low_back(n).start()

    table = table_ref[...]

    def row_ids(target_xl, e, first):
        return jnp.concatenate(
            [
                table + ((target_xl * 64 + z * 8 + ((first + j) % 4) * 2 + e) * CAP).astype(F32)
                for j in range(4)
            ],
            axis=0,
        )

    def pair_info(p, weights):
        a, b = PAIRS[p][0] % 8, PAIRS[p][1] % 8
        positions = jnp.concatenate([info_ref[a, 0:8], info_ref[b, 0:8] + FAR], axis=1)
        if not weights:
            return positions, None
        return positions, jnp.concatenate([info_ref[a, 8:16], info_ref[b, 8:16]], axis=1)

    def rows_of(hot, weight, p, chunk):
        a, b = PAIRS[p][0] % 8, PAIRS[p][1] % 8
        rows = nn(hot, jnp.concatenate([zb[a, chunk], zb[b, chunk]], axis=0))
        taken = rows[:, 0:512].astype(BF16)
        scaled = (rows[:, 512:1024] * weight).astype(BF16)
        return jnp.concatenate([taken, scaled], axis=1).reshape(4, 24, 1024)

    def select_diff(p, e):
        hot, weight = one_hot(row_ids(1 - xl, e, y), *pair_info(p, True))
        rows = rows_of(hot, weight, p, 0)
        relay[p, e, y] = rows[0]
        for j in range(1, 4):
            stage_diff[p, e, j - 1] = rows[j]
            diff_copy(p, e, j).start()

    def select_same(p, e, chunks):
        hot, weight = one_hot(row_ids(xl, e, y), *pair_info(p, True))
        for chunk in chunks:
            rows = rows_of(hot, weight, p, chunk)
            f_ref[core, xh if chunk == 0 else 1 - xh, e, p, xl, y] = rows[0]
            for j in range(1, 4):
                stage_same[p, e, j - 1, chunk] = rows[j]
                same_copy(p, e, j, chunk).start()

    def select_d(p):
        for e in (0, 1):
            select_diff(p, e)

    def select_a(p):
        for e in (0, 1):
            select_same(p, e, (0,))

    def select_b(p):
        for e in (0, 1):
            select_same(p, e, (1,))

    def select(p):
        for e in (0, 1):
            select_same(p, e, (0, 1))

    def forward_x(u):
        p, e = u // 2, u % 2
        drain(stage_diff.at[p, e], diff_recv.at[p, e])
        x_copy(p, e, 0).start()
        x_copy(p, e, 1).start()

    def forward_c(u):
        p, e = u // 2, u % 2
        drain(stage_same.at[p, e], same_recv.at[p, e])
        core_copy(p, e, 0).start()

    def forward(u):
        forward_x(u)
        forward_c(u)

    def gather(u):
        p, e = u // 2, u % 2
        for s in (0, 1):
            x_copy(p, e, 1 - s).wait_recv()
            core_copy(p, e, 1 + s).start()

    def compute(u):
        p, e = u // 2, u % 2
        for part in range(3):
            core_copy(p, e, part).wait_recv()

        def take(cq, qh, lo):
            return f_ref[cq, qh, e, p, :, :, :, lo : lo + 512].reshape(192, 512)

        x = jnp.concatenate([take(0, 0, 0), take(1, 0, 0), take(0, 1, 0), take(1, 1, 0)], axis=1)
        gate_in = jnp.concatenate([wg_ref[e], ag_ref[e]], axis=0)
        up_in = jnp.concatenate([wu_ref[e], au_ref[e]], axis=0)
        down_in = jnp.concatenate([wd_ref[e], bd_ref[e]], axis=0)
        gate = nt(x, gate_in)
        lg = gate[:, 192:256].astype(BF16)
        gate = gate[:, 0:192] + 0.5 * nn(lg, bg_ref[e])
        up_part = nt(x, up_in)
        lu = up_part[:, 192:256].astype(BF16)
        up_part = up_part[:, 0:192] + 0.5 * nn(lu, bu_ref[e])
        sigma = jax.nn.sigmoid(gate)
        active = gate * sigma
        hidden = (active * up_part).astype(BF16)
        down_part = nt(hidden, ad_ref[e]).astype(BF16)
        g = jnp.concatenate(
            [take(0, 0, 512), take(1, 0, 512), take(0, 1, 512), take(1, 1, 512)], axis=1
        )
        gh = nt(g, down_in)
        back = gh[:, 192:256].astype(BF16)
        gh = gh[:, 0:192] + 0.5 * nn(back, ad_ref[e])
        gg = (gh * up_part * sigma * (1.0 + gate * (1.0 - sigma))).astype(BF16)
        gu = (gh * active).astype(BF16)
        gp = nt(gg, bg_ref[e]).astype(BF16)
        upp = nt(gu, bu_ref[e]).astype(BF16)
        left = jnp.concatenate([gg, gp * 0.5], axis=1)
        right = jnp.concatenate([gu, upp * 0.5], axis=1)
        for q in range(4):
            cols = slice(q * 512, q * 512 + 512)
            part = nn(left, gate_in[:, cols]) + nn(right, up_in[:, cols])
            p_ref[q % 2, q // 2, e, p] = part.astype(BF16).reshape(2, 4, 24, 512)
        pc_copy(p, e).start()
        rows = slice(p * 192, p * 192 + 192)
        low_ref[e, rows, 0:64] = down_part
        low_ref[e, rows, 64:128] = gp
        low_ref[e, rows, 128:192] = upp
        for ref, value in ((gs_v, tn(lg, gg)), (us_v, tn(lu, gu)), (df_v, tn(back, hidden))):
            if p == 0:
                ref[e] = 0.5 * value
            else:
                ref[e] += 0.5 * value

    def chip_sum(u):
        p, e = u // 2, u % 2
        pc_copy(p, e).wait_recv()
        for n, qh, xs in ((0, 0, 1 - xl), (1, 1, 1 - xl), (2, 1 - xh, xl)):
            mine = p_ref[core, qh, e, p, xs].astype(F32)
            cpx[p, e, n] = (mine + r1[qh, e, p, xs].astype(F32)).astype(BF16)
        for n in range(3):
            px_copy(p, e, n).start()

    def x_sum(u):
        p, e = u // 2, u % 2
        drain(xr.at[p, e], px_recv.at[p, e])
        for j in range(4):
            to = (y + j) % 4
            same = p_ref[core, xh, e, p, xl, to].astype(F32) + r1[xh, e, p, xl, to].astype(F32)
            same = (same + xr[p, e, 2, to].astype(F32)).astype(BF16)
            diff = (xr[p, e, 0, to].astype(F32) + xr[p, e, 1, to].astype(F32)).astype(BF16)
            if j == 0:
                yr[p, 0, e, y] = same
                yr[p, 1, e, y] = diff
            else:
                back_stage[p, e, j - 1, 0] = same
                back_stage[p, e, j - 1, 1] = diff
                pd_copy(p, e, j).start()

    def combine(p):
        positions, _ = pair_info(p, False)
        hot = jnp.concatenate(
            [
                one_hot(row_ids(target_xl, e, 0), positions, None)
                for target_xl in (xl, 1 - xl)
                for e in (0, 1)
            ],
            axis=0,
        )
        drain(back_stage.at[p], pd_recv.at[p])
        t_ref[p] = tn(hot, yr[p].reshape(384, 512))

    held = {d: (p, i) for p in range(4) for i, d in enumerate(PAIRS[p])}

    def part_of(distance, chunk):
        p, i = held[distance]
        return t_ref[p, i * 128 + chunk * 64 : i * 128 + chunk * 64 + 64]

    def z_hop(direction, h, chunk):
        if h == 1 and chunk != direction:
            return
        n = direction * 4 + h - 1
        distance = 5 - h
        value = part_of(distance if direction == 0 or h == 1 else -distance, chunk)
        if h > 2 or (h == 2 and chunk == direction):
            z_copy(direction, h - 1, chunk).wait_recv()
            value = value + zr[n - 1, chunk].astype(F32)
        zs[n, chunk] = value.astype(BF16)
        z_copy(direction, h, chunk).start()


    def adapters(e):
        quarter = f_ref[core, xh, e].reshape(768, 1024)
        total = tl[e]
        both = 0.5 * tn(total[:, 64:192], quarter[:, 0:512])
        gf_v[e] = both[0:64]
        uf_v[e] = both[64:128]
        ds_v[e] = 0.5 * tn(total[:, 0:64], quarter[:, 512:1024])

    advance(1, 0)
    swap.wait_recv()
    ring(0, 1, 1).start()
    ring(1, 1, 1).start()
    select_d(0)
    select_a(0)
    forward_x(0)
    forward_x(1)
    advance(2, 0)
    select_d(1)
    gather(0)
    advance(1, 1)
    select_b(0)
    select_a(1)
    forward_x(2)
    forward_x(3)
    gather(1)
    forward_c(0)
    advance(3, 0)
    select_d(2)
    forward_c(1)
    for load in loads:
        load.wait()
    compute(0)
    advance(2, 1)
    select_b(1)
    forward_x(4)
    gather(2)
    chip_sum(0)
    compute(1)
    advance(4, 0)
    select_d(3)
    forward_x(5)
    gather(3)
    chip_sum(1)
    forward_c(2)
    advance(3, 1)
    select(2)
    forward_c(3)
    compute(2)
    forward_x(6)
    forward_x(7)
    gather(4)
    advance(4, 1)
    select(3)
    forward_c(4)
    compute(3)
    x_sum(0)
    chip_sum(2)
    gather(5)
    forward_c(5)
    compute(4)
    x_sum(1)
    chip_sum(3)
    gather(6)
    forward_c(6)
    compute(5)
    chip_sum(4)
    gather(7)
    forward_c(7)
    compute(6)
    x_sum(2)
    compute(7)
    low_core(0).start()
    low_core(1).start()
    chip_sum(6)
    x_sum(3)
    combine(0)
    chip_sum(7)
    chip_sum(5)
    for n, (src, dst) in enumerate(((gs_v, gs_ref), (us_v, us_ref), (df_v, df_ref))):
        put(n, src, dst)
    x_sum(4)
    combine(1)
    x_sum(6)
    x_sum(7)
    combine(3)
    z_hop(0, 1, 0)
    z_hop(1, 1, 1)
    x_sum(5)
    low_chip(0)
    low_chip(1)
    combine(2)
    for chunk in (1, 0):
        z_hop(0, 2, chunk)
        z_hop(1, 2, chunk)
    drain(zb.at[pl.ds(0, 7)], ring_send.at[0])
    drain(info_ref.at[pl.ds(0, 7)], info_send.at[0])
    swap.wait_send()
    drain(stage_same, same_send.at[0])
    drain(stage_diff, diff_send.at[0])
    drain(relay, x_send.at[0])
    drain(relay, x_send.at[1])
    drain(f_ref.at[0, :, :, :, 0], core_send.at[0])
    drain(f_ref.at[0, 0, :, :, 0], core_send.at[1])
    drain(f_ref.at[0, 0, :, :, 0], core_send.at[2])
    for chunk in (1, 0):
        z_hop(0, 3, chunk)
        z_hop(1, 3, chunk)
    low_total(0)
    low_total(1)
    for chunk in (1, 0):
        z_hop(0, 4, chunk)
        z_hop(1, 4, chunk)
    low_back(0).wait_recv()
    low_back(1).wait_recv()
    adapters(0)
    adapters(1)
    for n, (src, dst) in enumerate(((gf_v, gf_ref), (uf_v, uf_ref), (ds_v, ds_ref))):
        put(n + 3, src, dst)

    def home(chunk):
        z_copy(0, 4, chunk).wait_recv()
        z_copy(1, 4, chunk).wait_recv()
        return part_of(0, chunk) + zr[3, chunk].astype(F32) + zr[7, chunk].astype(F32)

    out_v[64:128] = home(1).astype(BF16)
    out_v[0:64] = home(0).astype(BF16)
    put(6, out_v, out_ref)
    drain(zs.at[pl.ds(0, 7)], z_send.at[0])
    drain(back_stage, pd_send.at[0])
    drain(cpx, px_send.at[0])
    drain(p_ref.at[0], pc_send.at[0])
    for n in (0, 1):
        low_core(n).wait_send()
        low_far(n).wait_send()
        low_back(n).wait_send()
    for copy in puts:
        copy.wait()


def step(tokens, grad_out, ids, weights, table, *frozen):
    vmem = pl.BlockSpec(memory_space=pltpu.VMEM)
    hbm = pl.BlockSpec(memory_space=pl.ANY)
    dma = pltpu.SemaphoreType.DMA

    def buf(*shape):
        return pltpu.VMEM(shape, BF16)

    return pl.pallas_call(
        kernel,
        name="experts",
        out_shape=(
            jax.ShapeDtypeStruct((128, 512), BF16),
            jax.ShapeDtypeStruct((2, 64, 512), F32),
            jax.ShapeDtypeStruct((2, 64, 192), F32),
            jax.ShapeDtypeStruct((2, 64, 512), F32),
            jax.ShapeDtypeStruct((2, 64, 192), F32),
            jax.ShapeDtypeStruct((2, 64, 192), F32),
            jax.ShapeDtypeStruct((2, 64, 512), F32),
        ),
        in_specs=[vmem] * 5 + [hbm] * 9,
        out_specs=(hbm,) * 7,
        scratch_shapes=[buf(*w.shape) for w in frozen] + [
            dma((9,)),
            pltpu.VMEM((8, 16, 128), F32),
            buf(8, 2, 128, 1024),
            buf(4, 2, 3, 2, 24, 1024),
            buf(4, 2, 3, 24, 1024),
            buf(4, 2, 4, 24, 1024),
            buf(2, 2, 2, 4, 2, 4, 24, 1024),
            buf(2, 2, 2, 4, 2, 4, 24, 512),
            buf(2, 2, 4, 2, 4, 24, 512),
            buf(4, 2, 3, 4, 24, 512),
            buf(4, 2, 3, 4, 24, 512),
            buf(4, 2, 3, 2, 24, 512),
            buf(4, 2, 2, 4, 24, 512),
            pltpu.VMEM((4, 256, 512), F32),
            buf(8, 2, 64, 512),
            buf(8, 2, 64, 512),
            buf(2, 768, 192),
            buf(768, 192),
            buf(768, 192),
            buf(768, 192),
            buf(2, 768, 192),
            dma((1,)), dma((2, 4)), dma((2,)), dma((1,)), dma((2, 8)),
            dma((1,)), dma((4, 2)), dma((1,)), dma((4, 2)),
            dma((2,)), dma((4, 2, 2)), dma((3,)), dma((4, 2, 3)),
            dma((1,)), dma((4, 2)), dma((1,)), dma((4, 2)), dma((1,)), dma((4,)),
            dma((1,)), dma((8, 2)), dma((3, 2)), dma((3, 2)), dma((7,)),
            buf(128, 512),
            *[pltpu.VMEM(shape, F32) for shape in (
                (2, 64, 512), (2, 64, 192), (2, 64, 512), (2, 64, 192), (2, 64, 192), (2, 64, 512),
            )],
        ],
        compiler_params=pltpu.CompilerParams(
            collective_id=0, has_side_effects=True, vmem_limit_bytes=VMEM_LIMIT
        ),
    )(tokens, grad_out, ids, weights, table, *frozen)


def finish_kernel(*refs):
    for src, dst in zip(refs[:7], refs[7:]):
        dst[...] = src[...]


def finish(outs):
    vmem = pl.BlockSpec(memory_space=pltpu.VMEM)
    return pl.pallas_call(
        finish_kernel,
        name="finish",
        out_shape=tuple(jax.ShapeDtypeStruct(o.shape, o.dtype) for o in outs),
        in_specs=[vmem] * 7,
        out_specs=(vmem,) * 7,
    )(*outs)


def local(tokens, grad_out, route_weights, expert_ids, wg, wu, wd, ag, bg, au, bu, ad, bd):
    row = np.arange(24)
    table = row % CAP + FAR * (row // CAP)
    table = jnp.asarray(table.reshape(24, 1), F32)
    wg, wu, ag, au, ad = [jnp.swapaxes(w, 1, 2) for w in (wg, wu, ag, au, ad)]
    outs = step(
        tokens, grad_out, expert_ids.T, route_weights.T, table, wg, wu, wd, ag, bg, au, bu, ad, bd
    )
    out, gf, gs, uf, us, df, ds = finish(outs)
    gf, uf, df = [jnp.swapaxes(w, 1, 2) for w in (gf, uf, df)]
    return out, gf, gs, uf, us, df, ds


def solution(mesh):
    specs = (
        P("expert", "tensor"), P("expert", "tensor"), P("expert", None), P("expert", None),
        P("expert", None, "tensor"), P("expert", None, "tensor"), P("expert", "tensor", None),
        P("expert", None, None), P("expert", None, "tensor"), P("expert", None, None),
        P("expert", None, "tensor"), P("expert", "tensor", None), P("expert", None, None),
    )
    outs = (
        P("expert", "tensor"), P("expert", "tensor", None), P("expert", None, "tensor"),
        P("expert", "tensor", None), P("expert", None, "tensor"), P("expert", "tensor", None),
        P("expert", None, "tensor"),
    )
    return jax.shard_map(local, mesh=mesh, in_specs=specs, out_specs=outs, check_vma=False)
```

```python
import functools

import jax
import jax.numpy as jnp
import numpy as np
from jax import lax
from jax.experimental import pallas as pl
from jax.experimental.pallas import tpu as pltpu
from jax.sharding import PartitionSpec as P

MESH = pl.DeviceIdType.MESH
F32 = jnp.float32
BF16 = jnp.bfloat16
PAIRS = ((0, 1), (-1, 2), (-2, 3), (-3, 4))
CAP = 12
FAR = 4096.0
VMEM_LIMIT = 67043328


def place():
    expert = lax.axis_index("expert")
    tensor = lax.axis_index("tensor")
    y = expert % 4
    z = (expert // 4) % 8
    xl = expert // 32
    xh = tensor // 2
    core = tensor % 2
    return xl, xh, y, z, core


def device(xl, xh, y, z, core):
    return (xl * 32 + z * 4 + y, xh * 2 + core)


def rem_copy(src, dst, send, recv, target):
    return pltpu.make_async_remote_copy(
        src_ref=src, dst_ref=dst, send_sem=send, recv_sem=recv,
        device_id=target, device_id_type=MESH,
    )


def drain(ref, sem):
    pltpu.make_async_copy(ref, ref, sem).wait()


def side(xl, xh, step):
    x = (xh * 2 + xl + step) % 4
    return x % 2, x // 2


def greet(targets):
    barrier = pltpu.get_barrier_semaphore()
    for target in targets:
        pl.semaphore_signal(barrier, inc=1, device_id=target, device_id_type=MESH)
    return barrier, len(targets)


def nt(a, b):
    return lax.dot_general(a, b, (((1,), (1,)), ((), ())), preferred_element_type=F32)


def tn(a, b):
    return lax.dot_general(a, b, (((0,), (0,)), ((), ())), preferred_element_type=F32)


def nn(a, b):
    return jnp.dot(a, b, preferred_element_type=F32)


def one_hot(ids, positions, weights):
    hot = jnp.zeros((96, 256), F32)
    weight = jnp.zeros((96, 256), F32)
    for k in range(8):
        match = ids == positions[k : k + 1]
        hot = jnp.where(match, 1.0, hot)
        if weights is not None:
            weight = jnp.where(match, weights[k : k + 1], weight)
    if weights is None:
        return hot.astype(BF16)
    return hot.astype(BF16), jnp.sum(weight, axis=1, keepdims=True)


def kernel(
    tok_ref, grad_ref, ids_ref, rw_ref, table_ref,
    wg_hbm, wu_hbm, wd_hbm, ag_hbm, bg_hbm, au_hbm, bu_hbm, ad_hbm, bd_hbm,
    out_ref, gf_ref, gs_ref, uf_ref, us_ref, df_ref, ds_ref,
    wg_ref, wu_ref, wd_ref, ag_ref, bg_ref, au_ref, bu_ref, ad_ref, bd_ref, w_sem,
    info_ref, zb, stage_same, stage_diff, relay, f_ref,
    p_ref, r1, cpx, xr, back_stage, yr, t_ref, zs, zr, low_ref, rl, ls, rl2, tl,
    info_send, info_recv, swap_sem, ring_send, ring_recv,
    same_send, same_recv, diff_send, diff_recv, x_send, x_recv, core_send, core_recv,
    pc_send, pc_recv, px_send, px_recv, pd_send, pd_recv,
    z_send, z_recv, l_send, l_recv, o_sem,
    out_v, gf_v, gs_v, uf_v, us_v, df_v, ds_v,
):
    xl, xh, y, z, core = place()
    here = functools.partial(device, xl, xh)
    y_others = [here((y + j) % 4, z, core) for j in range(1, 4)]
    x_sides = [device(*side(xl, xh, s), y, z, core) for s in (1, 3)]
    x_far = device(xl, 1 - xh, y, z, core)
    partner = here(y, z, 1 - core)
    down, up = here(y, (z + 7) % 8, core), here(y, (z + 1) % 8, core)

    greeted = greet([down, up] + y_others + x_sides + [x_far, partner])
    puts = []

    def put(n, src, dst):
        copy = pltpu.make_async_copy(src, dst, o_sem.at[n])
        copy.start()
        puts.append(copy)

    loads = []
    for n, (src, dst) in enumerate((
        (wg_hbm, wg_ref), (wu_hbm, wu_ref), (wd_hbm, wd_ref), (ag_hbm, ag_ref), (bg_hbm, bg_ref),
        (au_hbm, au_ref), (bu_hbm, bu_ref), (ad_hbm, ad_ref), (bd_hbm, bd_ref),
    )):
        load = pltpu.make_async_copy(src, dst, w_sem.at[n])
        load.start()
        loads.append(load)

    zb[0, 0, :, 0:512] = tok_ref[...]
    zb[0, 0, :, 512:1024] = grad_ref[...]

    ids = ids_ref[...]
    numbers = lax.broadcasted_iota(jnp.int32, (128, 128), 0)
    picked = jnp.zeros((128, 128), F32)
    for k in range(8):
        picked = jnp.where(ids[k : k + 1] == numbers, 1.0, picked)
    later = lax.broadcasted_iota(jnp.int32, (128, 128), 1) > numbers
    before = nn(picked.astype(BF16), jnp.where(later, 1.0, 0.0).astype(BF16))
    for k in range(8):
        slot = jnp.sum(jnp.where(ids[k : k + 1] == numbers, before, 0.0), axis=0, keepdims=True)
        info_ref[0, k : k + 1, :] = ids[k : k + 1].astype(F32) * CAP + slot
    info_ref[0, 8:16, :] = rw_ref[...]

    pl.semaphore_wait(*greeted)

    swap = rem_copy(zb.at[0, 0], zb.at[0, 1], swap_sem.at[0], swap_sem.at[1], x_far)
    swap.start()

    def ring(direction, h, chunk):
        if direction == 0:
            src, dst = (h - 1) % 8, h % 8
        else:
            src, dst = (1 - h) % 8, (-h) % 8
        n = (h - 1) * 2 + chunk
        return rem_copy(
            zb.at[src, chunk], zb.at[dst, chunk],
            ring_send.at[0], ring_recv.at[direction, n],
            down if direction == 0 else up,
        )

    def ring_info(direction, h):
        if direction == 0:
            src, dst = (h - 1) % 8, h % 8
        else:
            src, dst = (1 - h) % 8, (-h) % 8
        return rem_copy(
            info_ref.at[src], info_ref.at[dst],
            info_send.at[0], info_recv.at[direction, h - 1],
            down if direction == 0 else up,
        )

    def advance(h, chunk):
        for direction in (0, 1):
            if chunk == 0 and (h < 4 or direction == 0):
                ring_info(direction, h).wait_recv()
                if h < 3 or (h == 3 and direction == 0):
                    ring_info(direction, h + 1).start()
            if h < 4 or chunk == direction:
                ring(direction, h, chunk).wait_recv()
                if h < 3 or (h == 3 and chunk == direction):
                    ring(direction, h + 1, chunk).start()

    for direction in (0, 1):
        ring_info(direction, 1).start()
        ring(direction, 1, 0).start()
    def same_copy(p, e, j, chunk):
        qh = xh if chunk == 0 else 1 - xh
        return rem_copy(
            stage_same.at[p, e, j - 1, chunk], f_ref.at[core, qh, e, p, xl, y],
            same_send.at[0], same_recv.at[p, e],
            here((y + j) % 4, z, core),
        )

    def diff_copy(p, e, j):
        return rem_copy(
            stage_diff.at[p, e, j - 1], relay.at[p, e, y],
            diff_send.at[0], diff_recv.at[p, e], here((y + j) % 4, z, core),
        )

    def x_copy(p, e, s):
        return rem_copy(
            relay.at[p, e], f_ref.at[core, xh, e, p, xl],
            x_send.at[s], x_recv.at[p, e, s], x_sides[s],
        )

    def core_copy(p, e, part):
        if part == 0:
            piece = f_ref.at[core, :, e, p, xl]
        else:
            from_xl, from_xh = side(xl, xh, (1, 3)[part - 1])
            piece = f_ref.at[core, from_xh, e, p, from_xl]
        return rem_copy(piece, piece, core_send.at[part], core_recv.at[p, e, part], partner)

    def pc_copy(p, e):
        return rem_copy(
            p_ref.at[1 - core, :, e, p], r1.at[:, e, p], pc_send.at[0], pc_recv.at[p, e], partner
        )

    def pd_copy(p, e, j):
        return rem_copy(
            back_stage.at[p, e, j - 1], yr.at[p, :, e, y], pd_send.at[0], pd_recv.at[p],
            here((y + j) % 4, z, core),
        )

    def px_copy(p, e, s):
        if s == 2:
            src, dst, to = cpx.at[p, e, 2], xr.at[p, e, 2], x_far
        else:
            _, to_xh = side(xl, xh, (1, 3)[s])
            src, dst, to = cpx.at[p, e, to_xh], xr.at[p, e, xh], x_sides[s]
        return rem_copy(src, dst, px_send.at[0], px_recv.at[p, e], to)

    def z_copy(direction, h, chunk):
        n = direction * 4 + h - 1
        return rem_copy(
            zs.at[n, chunk], zr.at[n, chunk], z_send.at[0], z_recv.at[n, chunk],
            up if direction == 0 else down,
        )

    LOW = (slice(0, 576), slice(576, 768))

    def low_core(n):
        return rem_copy(
            low_ref.at[1 - core, LOW[n]], rl.at[LOW[n]], l_send.at[0, n], l_recv.at[0, n], partner
        )

    def low_far(n):
        return rem_copy(ls.at[LOW[n]], rl2.at[LOW[n]], l_send.at[1, n], l_recv.at[1, n], x_far)

    def low_back(n):
        return rem_copy(
            tl.at[core, LOW[n]], tl.at[core, LOW[n]], l_send.at[2, n], l_recv.at[2, n], partner
        )

    def low_chip(n):
        low_core(n).wait_recv()
        rows = LOW[n]
        ls[rows] = (low_ref[core, rows].astype(F32) + rl[rows].astype(F32)).astype(BF16)
        low_far(n).start()

    def low_total(n):
        low_far(n).wait_recv()
        rows = LOW[n]
        tl[core, rows] = (ls[rows].astype(F32) + rl2[rows].astype(F32)).astype(BF16)
        low_back(n).start()

    table = table_ref[...]

    def row_ids(target_xl, e, first):
        return jnp.concatenate(
            [
                table + ((target_xl * 64 + z * 8 + ((first + j) % 4) * 2 + e) * CAP).astype(F32)
                for j in range(4)
            ],
            axis=0,
        )

    def pair_info(p, weights):
        a, b = PAIRS[p][0] % 8, PAIRS[p][1] % 8
        positions = jnp.concatenate([info_ref[a, 0:8], info_ref[b, 0:8] + FAR], axis=1)
        if not weights:
            return positions, None
        return positions, jnp.concatenate([info_ref[a, 8:16], info_ref[b, 8:16]], axis=1)

    def rows_of(hot, weight, p, chunk):
        a, b = PAIRS[p][0] % 8, PAIRS[p][1] % 8
        rows = nn(hot, jnp.concatenate([zb[a, chunk], zb[b, chunk]], axis=0))
        taken = rows[:, 0:512].astype(BF16)
        scaled = (rows[:, 512:1024] * weight).astype(BF16)
        return jnp.concatenate([taken, scaled], axis=1).reshape(4, 24, 1024)

    def select_diff(p, e):
        hot, weight = one_hot(row_ids(1 - xl, e, y), *pair_info(p, True))
        rows = rows_of(hot, weight, p, 0)
        relay[p, e, y] = rows[0]
        for j in range(1, 4):
            stage_diff[p, e, j - 1] = rows[j]
            diff_copy(p, e, j).start()

    def select_same(p, e, chunks):
        hot, weight = one_hot(row_ids(xl, e, y), *pair_info(p, True))
        for chunk in chunks:
            rows = rows_of(hot, weight, p, chunk)
            f_ref[core, xh if chunk == 0 else 1 - xh, e, p, xl, y] = rows[0]
            for j in range(1, 4):
                stage_same[p, e, j - 1, chunk] = rows[j]
                same_copy(p, e, j, chunk).start()

    def select_d(p):
        for e in (0, 1):
            select_diff(p, e)

    def select_a(p):
        for e in (0, 1):
            select_same(p, e, (0,))

    def select_b(p):
        for e in (0, 1):
            select_same(p, e, (1,))

    def select(p):
        for e in (0, 1):
            select_same(p, e, (0, 1))

    def forward_x(u):
        p, e = u // 2, u % 2
        drain(stage_diff.at[p, e], diff_recv.at[p, e])
        x_copy(p, e, 0).start()
        x_copy(p, e, 1).start()

    def forward_c(u):
        p, e = u // 2, u % 2
        drain(stage_same.at[p, e], same_recv.at[p, e])
        core_copy(p, e, 0).start()

    def forward(u):
        forward_x(u)
        forward_c(u)

    def gather(u):
        p, e = u // 2, u % 2
        for s in (0, 1):
            x_copy(p, e, 1 - s).wait_recv()
            core_copy(p, e, 1 + s).start()

    def compute(u):
        p, e = u // 2, u % 2
        for part in range(3):
            core_copy(p, e, part).wait_recv()

        def take(cq, qh, lo):
            return f_ref[cq, qh, e, p, :, :, :, lo : lo + 512].reshape(192, 512)

        x = jnp.concatenate([take(0, 0, 0), take(1, 0, 0), take(0, 1, 0), take(1, 1, 0)], axis=1)
        gate_in = jnp.concatenate([wg_ref[e], ag_ref[e]], axis=0)
        up_in = jnp.concatenate([wu_ref[e], au_ref[e]], axis=0)
        down_in = jnp.concatenate([wd_ref[e], bd_ref[e]], axis=0)
        gate = nt(x, gate_in)
        lg = gate[:, 192:256].astype(BF16)
        gate = gate[:, 0:192] + 0.5 * nn(lg, bg_ref[e])
        up_part = nt(x, up_in)
        lu = up_part[:, 192:256].astype(BF16)
        up_part = up_part[:, 0:192] + 0.5 * nn(lu, bu_ref[e])
        sigma = jax.nn.sigmoid(gate)
        active = gate * sigma
        hidden = (active * up_part).astype(BF16)
        down_part = nt(hidden, ad_ref[e]).astype(BF16)
        g = jnp.concatenate(
            [take(0, 0, 512), take(1, 0, 512), take(0, 1, 512), take(1, 1, 512)], axis=1
        )
        gh = nt(g, down_in)
        back = gh[:, 192:256].astype(BF16)
        gh = gh[:, 0:192] + 0.5 * nn(back, ad_ref[e])
        gg = (gh * up_part * sigma * (1.0 + gate * (1.0 - sigma))).astype(BF16)
        gu = (gh * active).astype(BF16)
        gp = nt(gg, bg_ref[e]).astype(BF16)
        upp = nt(gu, bu_ref[e]).astype(BF16)
        left = jnp.concatenate([gg, gp * 0.5], axis=1)
        right = jnp.concatenate([gu, upp * 0.5], axis=1)
        for q in range(4):
            cols = slice(q * 512, q * 512 + 512)
            part = nn(left, gate_in[:, cols]) + nn(right, up_in[:, cols])
            p_ref[q % 2, q // 2, e, p] = part.astype(BF16).reshape(2, 4, 24, 512)
        pc_copy(p, e).start()
        rows = slice(p * 192, p * 192 + 192)
        low_ref[e, rows, 0:64] = down_part
        low_ref[e, rows, 64:128] = gp
        low_ref[e, rows, 128:192] = upp
        for ref, value in ((gs_v, tn(lg, gg)), (us_v, tn(lu, gu)), (df_v, tn(back, hidden))):
            if p == 0:
                ref[e] = 0.5 * value
            else:
                ref[e] += 0.5 * value

    def chip_sum(u):
        p, e = u // 2, u % 2
        pc_copy(p, e).wait_recv()
        for n, qh, xs in ((0, 0, 1 - xl), (1, 1, 1 - xl), (2, 1 - xh, xl)):
            mine = p_ref[core, qh, e, p, xs].astype(F32)
            cpx[p, e, n] = (mine + r1[qh, e, p, xs].astype(F32)).astype(BF16)
        for n in range(3):
            px_copy(p, e, n).start()

    def x_sum(u):
        p, e = u // 2, u % 2
        drain(xr.at[p, e], px_recv.at[p, e])
        for j in range(4):
            to = (y + j) % 4
            same = p_ref[core, xh, e, p, xl, to].astype(F32) + r1[xh, e, p, xl, to].astype(F32)
            same = (same + xr[p, e, 2, to].astype(F32)).astype(BF16)
            diff = (xr[p, e, 0, to].astype(F32) + xr[p, e, 1, to].astype(F32)).astype(BF16)
            if j == 0:
                yr[p, 0, e, y] = same
                yr[p, 1, e, y] = diff
            else:
                back_stage[p, e, j - 1, 0] = same
                back_stage[p, e, j - 1, 1] = diff
                pd_copy(p, e, j).start()

    def combine(p):
        positions, _ = pair_info(p, False)
        hot = jnp.concatenate(
            [
                one_hot(row_ids(target_xl, e, 0), positions, None)
                for target_xl in (xl, 1 - xl)
                for e in (0, 1)
            ],
            axis=0,
        )
        drain(back_stage.at[p], pd_recv.at[p])
        t_ref[p] = tn(hot, yr[p].reshape(384, 512))

    held = {d: (p, i) for p in range(4) for i, d in enumerate(PAIRS[p])}

    def part_of(distance, chunk):
        p, i = held[distance]
        return t_ref[p, i * 128 + chunk * 64 : i * 128 + chunk * 64 + 64]

    def z_hop(direction, h, chunk):
        if h == 1 and chunk != direction:
            return
        n = direction * 4 + h - 1
        distance = 5 - h
        value = part_of(distance if direction == 0 or h == 1 else -distance, chunk)
        if h > 2 or (h == 2 and chunk == direction):
            z_copy(direction, h - 1, chunk).wait_recv()
            value = value + zr[n - 1, chunk].astype(F32)
        zs[n, chunk] = value.astype(BF16)
        z_copy(direction, h, chunk).start()


    def adapters(e):
        quarter = f_ref[core, xh, e].reshape(768, 1024)
        total = tl[e]
        both = 0.5 * tn(total[:, 64:192], quarter[:, 0:512])
        gf_v[e] = both[0:64]
        uf_v[e] = both[64:128]
        ds_v[e] = 0.5 * tn(total[:, 0:64], quarter[:, 512:1024])

    advance(1, 0)
    swap.wait_recv()
    ring(0, 1, 1).start()
    ring(1, 1, 1).start()
    select_d(0)
    select_a(0)
    forward_x(0)
    forward_x(1)
    advance(2, 0)
    select_d(1)
    gather(0)
    advance(1, 1)
    select_b(0)
    select_a(1)
    forward_x(2)
    forward_x(3)
    gather(1)
    forward_c(0)
    advance(3, 0)
    select_d(2)
    forward_c(1)
    for load in loads:
        load.wait()
    compute(0)
    advance(2, 1)
    select_b(1)
    forward_x(4)
    gather(2)
    chip_sum(0)
    compute(1)
    advance(4, 0)
    select_d(3)
    forward_x(5)
    gather(3)
    chip_sum(1)
    forward_c(2)
    advance(3, 1)
    select(2)
    forward_c(3)
    compute(2)
    forward_x(6)
    forward_x(7)
    gather(4)
    advance(4, 1)
    select(3)
    forward_c(4)
    compute(3)
    x_sum(0)
    chip_sum(2)
    gather(5)
    forward_c(5)
    compute(4)
    x_sum(1)
    chip_sum(3)
    gather(6)
    forward_c(6)
    compute(5)
    chip_sum(4)
    gather(7)
    forward_c(7)
    compute(6)
    x_sum(2)
    compute(7)
    low_core(0).start()
    low_core(1).start()
    chip_sum(6)
    x_sum(3)
    combine(0)
    chip_sum(7)
    chip_sum(5)
    for n, (src, dst) in enumerate(((gs_v, gs_ref), (us_v, us_ref), (df_v, df_ref))):
        put(n, src, dst)
    x_sum(4)
    combine(1)
    x_sum(6)
    x_sum(7)
    combine(3)
    z_hop(0, 1, 0)
    z_hop(1, 1, 1)
    x_sum(5)
    low_chip(0)
    low_chip(1)
    combine(2)
    for chunk in (1, 0):
        z_hop(0, 2, chunk)
        z_hop(1, 2, chunk)
    drain(zb.at[pl.ds(0, 7)], ring_send.at[0])
    drain(info_ref.at[pl.ds(0, 7)], info_send.at[0])
    swap.wait_send()
    drain(stage_same, same_send.at[0])
    drain(stage_diff, diff_send.at[0])
    drain(relay, x_send.at[0])
    drain(relay, x_send.at[1])
    drain(f_ref.at[0, :, :, :, 0], core_send.at[0])
    drain(f_ref.at[0, 0, :, :, 0], core_send.at[1])
    drain(f_ref.at[0, 0, :, :, 0], core_send.at[2])
    for chunk in (1, 0):
        z_hop(0, 3, chunk)
        z_hop(1, 3, chunk)
    low_total(0)
    low_total(1)
    for chunk in (1, 0):
        z_hop(0, 4, chunk)
        z_hop(1, 4, chunk)
    low_back(0).wait_recv()
    low_back(1).wait_recv()
    adapters(0)
    adapters(1)
    for n, (src, dst) in enumerate(((gf_v, gf_ref), (uf_v, uf_ref), (ds_v, ds_ref))):
        put(n + 3, src, dst)

    def home(chunk):
        z_copy(0, 4, chunk).wait_recv()
        z_copy(1, 4, chunk).wait_recv()
        return part_of(0, chunk) + zr[3, chunk].astype(F32) + zr[7, chunk].astype(F32)

    out_v[64:128] = home(1).astype(BF16)
    out_v[0:64] = home(0).astype(BF16)
    put(6, out_v, out_ref)
    drain(zs.at[pl.ds(0, 7)], z_send.at[0])
    drain(back_stage, pd_send.at[0])
    drain(cpx, px_send.at[0])
    drain(p_ref.at[0], pc_send.at[0])
    for n in (0, 1):
        low_core(n).wait_send()
        low_far(n).wait_send()
        low_back(n).wait_send()
    for copy in puts:
        copy.wait()


def step(tokens, grad_out, ids, weights, table, *frozen):
    vmem = pl.BlockSpec(memory_space=pltpu.VMEM)
    hbm = pl.BlockSpec(memory_space=pl.ANY)
    dma = pltpu.SemaphoreType.DMA

    def buf(*shape):
        return pltpu.VMEM(shape, BF16)

    return pl.pallas_call(
        kernel,
        name="experts",
        out_shape=(
            jax.ShapeDtypeStruct((128, 512), BF16),
            jax.ShapeDtypeStruct((2, 64, 512), F32),
            jax.ShapeDtypeStruct((2, 64, 192), F32),
            jax.ShapeDtypeStruct((2, 64, 512), F32),
            jax.ShapeDtypeStruct((2, 64, 192), F32),
            jax.ShapeDtypeStruct((2, 64, 192), F32),
            jax.ShapeDtypeStruct((2, 64, 512), F32),
        ),
        in_specs=[vmem] * 5 + [hbm] * 9,
        out_specs=(hbm,) * 7,
        scratch_shapes=[buf(*w.shape) for w in frozen] + [
            dma((9,)),
            pltpu.VMEM((8, 16, 128), F32),
            buf(8, 2, 128, 1024),
            buf(4, 2, 3, 2, 24, 1024),
            buf(4, 2, 3, 24, 1024),
            buf(4, 2, 4, 24, 1024),
            buf(2, 2, 2, 4, 2, 4, 24, 1024),
            buf(2, 2, 2, 4, 2, 4, 24, 512),
            buf(2, 2, 4, 2, 4, 24, 512),
            buf(4, 2, 3, 4, 24, 512),
            buf(4, 2, 3, 4, 24, 512),
            buf(4, 2, 3, 2, 24, 512),
            buf(4, 2, 2, 4, 24, 512),
            pltpu.VMEM((4, 256, 512), F32),
            buf(8, 2, 64, 512),
            buf(8, 2, 64, 512),
            buf(2, 768, 192),
            buf(768, 192),
            buf(768, 192),
            buf(768, 192),
            buf(2, 768, 192),
            dma((1,)), dma((2, 4)), dma((2,)), dma((1,)), dma((2, 8)),
            dma((1,)), dma((4, 2)), dma((1,)), dma((4, 2)),
            dma((2,)), dma((4, 2, 2)), dma((3,)), dma((4, 2, 3)),
            dma((1,)), dma((4, 2)), dma((1,)), dma((4, 2)), dma((1,)), dma((4,)),
            dma((1,)), dma((8, 2)), dma((3, 2)), dma((3, 2)), dma((7,)),
            buf(128, 512),
            *[pltpu.VMEM(shape, F32) for shape in (
                (2, 64, 512), (2, 64, 192), (2, 64, 512), (2, 64, 192), (2, 64, 192), (2, 64, 512),
            )],
        ],
        compiler_params=pltpu.CompilerParams(
            collective_id=0, has_side_effects=True, vmem_limit_bytes=VMEM_LIMIT
        ),
    )(tokens, grad_out, ids, weights, table, *frozen)


def finish_kernel(*refs):
    for src, dst in zip(refs[:7], refs[7:]):
        dst[...] = src[...]


def finish(outs):
    vmem = pl.BlockSpec(memory_space=pltpu.VMEM)
    return pl.pallas_call(
        finish_kernel,
        name="finish",
        out_shape=tuple(jax.ShapeDtypeStruct(o.shape, o.dtype) for o in outs),
        in_specs=[vmem] * 7,
        out_specs=(vmem,) * 7,
    )(*outs)


def local(tokens, grad_out, route_weights, expert_ids, wg, wu, wd, ag, bg, au, bu, ad, bd):
    row = np.arange(24)
    table = row % CAP + FAR * (row // CAP)
    table = jnp.asarray(table.reshape(24, 1), F32)
    wg, wu, ag, au, ad = [jnp.swapaxes(w, 1, 2) for w in (wg, wu, ag, au, ad)]
    outs = step(
        tokens, grad_out, expert_ids.T, route_weights.T, table, wg, wu, wd, ag, bg, au, bu, ad, bd
    )
    out, gf, gs, uf, us, df, ds = finish(outs)
    gf, uf, df = [jnp.swapaxes(w, 1, 2) for w in (gf, uf, df)]
    return out, gf, gs, uf, us, df, ds


def solution(mesh):
    specs = (
        P("expert", "tensor"), P("expert", "tensor"), P("expert", None), P("expert", None),
        P("expert", None, "tensor"), P("expert", None, "tensor"), P("expert", "tensor", None),
        P("expert", None, None), P("expert", None, "tensor"), P("expert", None, None),
        P("expert", None, "tensor"), P("expert", "tensor", None), P("expert", None, None),
    )
    outs = (
        P("expert", "tensor"), P("expert", "tensor", None), P("expert", None, "tensor"),
        P("expert", "tensor", None), P("expert", None, "tensor"), P("expert", "tensor", None),
        P("expert", None, "tensor"),
    )
    return jax.shard_map(local, mesh=mesh, in_specs=specs, out_specs=outs, check_vma=False)
```
